32 devices in a mesh: gx: 4 (over y, x), gy: 8 (over z, core).
Axes of the slice: x: 2, y: 2, z: 4, core: 2. Of those that a mesh axis runs over, the one named last changes fastest.
Arguments:
- velocity: float32 [3, 48, 224, 1024], P(None, 'gx', 'gy'), may hold values from -12 to 12
- viscosity: float32 [48, 224, 1024], P('gx', 'gy'), may hold values from 0.5 to 4
- cells: int32 [3, 32768], P(None, ('gx', 'gy')), may hold values from 0 to 1023, as said below
- offsets: float32 [3, 32768], P(None, ('gx', 'gy')), may hold values from 0 to 1
- forces: float32 [3, 32768], P(None, ('gx', 'gy')), may hold values from -48 to 48
- owners: int32 [32768, 1], P(('gx', 'gy')), may hold values from 0 to 31; in each aligned block of 1024 rows (0 to 1023, 1024 to 2047, ...) at most 64 rows name the same one
Outputs:
- new_velocity: float32 [3, 48, 224, 1024], P(None, 'gx', 'gy')
- marker_velocity: float32 [3, 32768], P(None, ('gx', 'gy'))
The draws below stay inside these ranges and needn't reach their ends.
Inputs may be any that keep to these rules, and one draw needn't show every extreme that they name: cells[0] lies below 12, cells[1] below 28, cells[2] below 1024. `owners`: among one device's 1024 markers at most 64 have the same owner, and in every draw some owner is named exactly 64 times by one device's markers.
All inputs are finite; a program needn't handle non-finite values.
Results may differ from the reference program's by a relative error of at most 0.000096.
Values sent between devices are 32-bit elements; how exact they have to be, the bound alone decides.
A program may use at most 128 MiB of HBM per device.

```python
import math
import jax
import jax.numpy as jnp
import numpy as np

CX = 12
CY = 28
NZ = 1024
M_DEV = 1024
SWEEPS = 3
NX = 48
NY = 224
MARKERS = 32768
CAP = 64
N_GY = 8
DEVICES = 32


def draw_cells(key, part):
    upper = jnp.array([[CX], [CY], [NZ]], jnp.int32)
    return jax.random.randint(key, (3, MARKERS), 0, upper, dtype=jnp.int32)


def block_levels(own_key, extent, cuts, smallest, largest):
    loudness, own = 1.0, jax.random.fold_in(own_key, 6)
    for axis_at, blocks in cuts:
        draws = jnp.exp(jax.random.uniform(jax.random.fold_in(own, axis_at), (blocks,), jnp.float32, smallest / len(cuts), largest / len(cuts)))
        loudness = loudness * jnp.repeat(draws, extent[axis_at] // blocks).reshape([-1 if axis == axis_at else 1 for axis in range(len(extent))])
    return loudness


def assign_block(key, own, number, rows, amount, top, bound, skew):
    order = jax.random.permutation(key, amount)
    heavy_load, ordinary = portions_of(amount, rows * top, bound, skew, True), portions_of(amount, rows * top, bound, skew, False)
    places = jnp.arange(amount)

    def named(tallies, turn):
        used = int((tallies > 0).sum())
        fixed = max(1, used // 4)
        moved = fixed + (places - fixed + turn * (used - fixed)) % max(1, amount - fixed)
        return jnp.zeros((amount,), jnp.int32).at[order[jnp.where(places < fixed, places, moved)]].set(jnp.asarray(tallies, jnp.int32))

    tallies = jnp.where(number % 4 == 0, named(heavy_load, number // 4), named(ordinary, number - number // 4 - 1))
    mixed = jax.random.permutation(jax.random.fold_in(own, 3), amount)
    donor, taker = mixed[0:amount // 2 * 2:2], mixed[1:amount // 2 * 2:2]
    margin = jnp.minimum(tallies[donor] - 1, bound - tallies[taker]) // 2
    margin = jnp.where((donor == order[0]) | (taker == order[0]) | (tallies[taker] == 0), 0, jnp.maximum(margin, 0))
    moved = jax.random.randint(jax.random.fold_in(own, 4), (amount // 2,), 0, 1 << 20) % (margin + 1)
    tallies = tallies.at[donor].add(-moved).at[taker].add(moved)
    labels = jnp.searchsorted(jnp.cumsum(tallies), jnp.arange(rows * top), side="right").astype(jnp.int32)
    grid = labels.reshape(top, rows).T
    grid = grid[jax.random.permutation(jax.random.fold_in(own, 1), rows)]
    turn = jax.random.randint(jax.random.fold_in(own, 2), (rows, 1), 0, top)
    return jnp.take_along_axis(grid, (jnp.arange(top)[None, :] + turn) % top, axis=1)


def portions_of(count, total, limit, slope, full):
    weights = [(1 << 20) // math.isqrt(grade ** slope) + 1 for grade in range(1, count + 1)]
    largest = limit if full else min(limit, max(-(-total // count), total * weights[0] // sum(weights)))
    least = 1 if total - largest >= count - 1 else 0
    counts, rest = [largest] + [least] * (count - 1), total - largest - least * (count - 1)
    while rest > 0:
        free = [i for i in range(1, count) if counts[i] < largest] or [i for i in range(1, count) if counts[i] < limit]
        whole, left = sum([weights[i] for i in free]), rest
        for i in free:
            more = min(limit - counts[i], max(1, left * weights[i] // whole), rest)
            counts[i] = counts[i] + more
            rest = rest - more
    return np.array(counts)


def bell_draw(key, shape, spread, reach, cuts=(), kind=jnp.bfloat16):
    level = block_levels(key, shape, cuts, -0.22, 0.18) if cuts else 1.0
    drawn = jax.random.normal(key, shape, jnp.float32) * spread * level
    return jnp.minimum(jnp.maximum(drawn, -reach), reach).astype(kind)


def setup_inputs(seed: int = 0) -> dict:
    key_of = jax.random.split(jax.random.key(seed), 7)
    velocity = bell_draw(key_of[0], (3, NX, NY, NZ), 2.0, 12.0, ((1, 4), (2, 8)), jnp.float32)
    viscosity = jnp.clip(jnp.exp(math.log(4.0) - 2.0794415 * jax.random.uniform(key_of[1], (NX, NY, NZ), jnp.float32) ** block_levels(key_of[1], (NX, NY, NZ), ((0, 4), (1, 8)), -0.2, 0.2)), 0.5, 4.0)
    cells = draw_cells(jax.random.fold_in(key_of[6], 71), 0)
    offsets = jnp.clip(1.0 * jax.random.uniform(key_of[3], (3, MARKERS), jnp.float32) ** block_levels(key_of[3], (3, MARKERS), ((1, 32),), -0.2, 0.2), 0.0, 1.0)
    forces = bell_draw(key_of[4], (3, MARKERS), 8.0, 48.0, ((1, 32),), jnp.float32)
    owners_keys = jax.random.split(jax.random.fold_in(key_of[5], 1), MARKERS // M_DEV)
    owners_turns = jax.random.permutation(jax.random.fold_in(key_of[5], 3), MARKERS // M_DEV)
    owners = jax.vmap(lambda own, number: assign_block(jax.random.fold_in(key_of[5], 2), own, number, M_DEV, DEVICES, 1, CAP, 2))(owners_keys, owners_turns).reshape((MARKERS, 1))
    return dict(velocity=velocity, viscosity=viscosity, cells=cells, offsets=offsets, forces=forces, owners=owners)


def kernel_weights(frac):
    root = jnp.sqrt(1.0 + 4.0 * frac - 4.0 * frac * frac)
    return jnp.stack([(3.0 - 2.0 * frac - root) / 8.0, (3.0 - 2.0 * frac + root) / 8.0, (1.0 + 2.0 * frac + root) / 8.0, (1.0 + 2.0 * frac - root) / 8.0])

def reference(velocity, viscosity, cells, offsets, forces, owners):
    owner = owners[:, 0]
    base_x = owner // N_GY * CX + cells[0]
    base_y = owner % N_GY * CY + cells[1]
    base_z = cells[2]
    weight_x = kernel_weights(offsets[0])
    weight_y = kernel_weights(offsets[1])
    weight_z = kernel_weights(offsets[2])
    flat = jnp.zeros((3, NX * NY * NZ), jnp.float32)
    entries = []
    for i in range(4):
        for j in range(4):
            for k in range(4):
                index = (((base_x - 1 + i) % NX * NY + (base_y - 1 + j) % NY) * NZ + (base_z - 1 + k) % NZ).astype(jnp.int32)
                weight = weight_x[i] * weight_y[j] * weight_z[k]
                entries.append((index, weight))
                flat = flat.at[:, index].add(forces * weight[None, :])
    rhs = velocity + flat.reshape(3, NX, NY, NZ)
    field = rhs
    for sweep in range(SWEEPS):
        beside_all = jnp.roll(field, -1, 1) + jnp.roll(field, 1, 1)
        beside_all = beside_all + jnp.roll(field, -1, 2) + jnp.roll(field, 1, 2)
        beside_all = beside_all + jnp.roll(field, -1, 3) + jnp.roll(field, 1, 3)
        field = (rhs + viscosity * beside_all) / (1.0 + 6.0 * viscosity)
    values = field.reshape(3, NX * NY * NZ)
    speeds = jnp.zeros((3, owner.shape[0]), jnp.float32)
    for index, weight in entries:
        speeds = speeds + values[:, index] * weight[None, :]
    return (field, speeds)
```

```python
import functools

import jax
import jax.numpy as jnp
from jax import lax
from jax.experimental import pallas as pl
from jax.experimental.pallas import tpu as pltpu
from jax.sharding import PartitionSpec as P

MESH = pl.DeviceIdType.MESH

SWEEPS = 3
LANES = 128
FIELDS = 16


def shifted(block, axis, step):
    count = lax.axis_size(axis)
    return lax.ppermute(block, axis, [(i, (i + step) % count) for i in range(count)])


def kernel_weights(frac):
    root = jnp.sqrt(1.0 + 4.0 * frac - 4.0 * frac * frac)
    return (
        (3.0 - 2.0 * frac - root) * 0.125,
        (3.0 - 2.0 * frac + root) * 0.125,
        (1.0 + 2.0 * frac + root) * 0.125,
        (1.0 + 2.0 * frac - root) * 0.125,
    )


def exchange_kernel(out_ref, in_ref, send_sem, recv_sem):
    count_x, count_y = lax.axis_size("gx"), lax.axis_size("gy")
    devices = count_x * count_y
    me = lax.axis_index("gx") * count_y + lax.axis_index("gy")

    def place(index):
        return (lax.div(index, count_y), lax.rem(index, count_y))

    barrier = pltpu.get_barrier_semaphore()

    def greet(k, carry):
        pl.semaphore_signal(
            barrier, inc=1, device_id=place(lax.rem(me + k, devices)), device_id_type=MESH
        )
        return carry

    lax.fori_loop(1, devices, greet, 0)
    pl.semaphore_wait(barrier, devices - 1)

    def copy(k, source, target):
        return pltpu.make_async_remote_copy(
            src_ref=out_ref.at[target], dst_ref=in_ref.at[source],
            send_sem=send_sem.at[k], recv_sem=recv_sem.at[k],
            device_id=place(target), device_id_type=MESH,
        )

    def begin(k, carry):
        copy(k, me, lax.rem(me + k, devices)).start()
        return carry

    def finish(k, carry):
        target = lax.rem(me + k, devices)
        source = lax.rem(me + devices - k, devices)
        copy(k, me, target).wait_send()
        copy(k, source, target).wait_recv()
        return carry

    lax.fori_loop(1, devices, begin, 0)
    in_ref[me] = out_ref[me]
    lax.fori_loop(1, devices, finish, 0)


def exchanged(values, count, collective_id):
    devices = lax.axis_size("gx") * lax.axis_size("gy")
    rows = values.shape[0]
    tile = 8 * LANES
    sized = -(-rows * count // tile) * tile
    flat = values.reshape(rows, devices, count).transpose(1, 0, 2).reshape(devices, rows * count)
    flat = jnp.pad(flat, ((0, 0), (0, sized - rows * count)))
    flat = flat.reshape(devices, sized // LANES, LANES)
    received = pl.pallas_call(
        exchange_kernel,
        out_shape=jax.ShapeDtypeStruct(flat.shape, jnp.float32),
        in_specs=[pl.BlockSpec(memory_space=pltpu.VMEM)],
        out_specs=pl.BlockSpec(memory_space=pltpu.VMEM),
        scratch_shapes=[pltpu.SemaphoreType.DMA((devices,)), pltpu.SemaphoreType.DMA((devices,))],
        compiler_params=pltpu.CompilerParams(collective_id=collective_id, has_side_effects=True),
    )(flat)
    received = received.reshape(devices, sized)[:, : rows * count].reshape(devices, rows, count)
    return received.transpose(1, 0, 2).reshape(rows, devices * count)


def tent(first, weights, length, wrap=0):
    rows = lax.broadcasted_iota(jnp.int32, (length, LANES), 0)
    table = jnp.zeros((length, LANES), jnp.float32)
    for j in range(4):
        target = first + j
        if wrap:
            target = jnp.where(target < 0, target + wrap, target)
            target = jnp.where(target >= wrap, target - wrap, target)
        table = table + jnp.where(rows == target, weights[j], 0.0)
    return table


def halves(value):
    high = value.astype(jnp.bfloat16)
    low = (value - high.astype(jnp.float32)).astype(jnp.bfloat16)
    return high, low


def chunk_tables(part, tile, x_shift, layers, ext_y, depth):
    cells = part[0:3].astype(jnp.int32)
    table_x = tent(cells[0:1] + x_shift, kernel_weights(part[3:4]), layers)
    table_y = tent(cells[1:2] - 1, kernel_weights(part[4:5]), ext_y, ext_y)
    start = cells[2:3] - 1
    start = jnp.where(start < 0, start + depth, start) - tile * LANES
    table_z = tent(start, kernel_weights(part[5:6]), 2 * LANES)
    return table_x, table_y, table_z


def lanes_of(tile):
    return pl.ds(pl.multiple_of(tile * LANES, LANES), LANES)


def transposed_dot(left, right):
    return lax.dot_general(
        left, right, (((1,), (1,)), ((), ())), preferred_element_type=jnp.float32
    )


def spread_kernel(
    size_x, size_y, ext_y, depth, meta_ref, own_ref, low_ref, high_ref, out_ref, up_ref, down_ref
):
    layers = size_x + 2
    tiles = depth // LANES

    def clear(i, carry):
        for c in range(3):
            out_ref[c, i] = jnp.zeros((ext_y, depth), jnp.float32)
        return carry

    lax.fori_loop(0, layers, clear, 0)

    def add(which, ref, x_shift, first, last):
        def chunk(j, carry):
            tile = meta_ref[which, j + 1]
            after = lax.rem(tile + 1, tiles)
            part = ref[:, lanes_of(j)]
            table_x, table_y, table_z = chunk_tables(part, tile, x_shift, FIELDS, ext_y, depth)
            z_high, z_low = halves(table_z)
            z_pair = jnp.concatenate([z_high, z_high], axis=1)
            for c in range(3):
                pushed = table_x * part[6 + c : 7 + c]
                planes = jnp.concatenate(
                    [pushed[x : x + 1] * table_y for x in range(first, last)], axis=0
                )
                high, low = halves(planes)
                total = transposed_dot(jnp.concatenate([high, low], axis=1), z_pair)
                total = total + transposed_dot(high, z_low)
                shape = (last - first, ext_y, LANES)
                out_ref[c, first:last, :, lanes_of(tile)] += total[:, :LANES].reshape(shape)
                out_ref[c, first:last, :, lanes_of(after)] += total[:, LANES:].reshape(shape)
            return carry

        lax.fori_loop(0, meta_ref[which, 0], chunk, 0)

    add(0, own_ref, 0, 0, layers)
    add(1, low_ref, -size_x, 0, 3)
    add(2, high_ref, size_x, layers - 2, layers)

    def pack(x, carry):
        for c in range(3):
            for k, row in enumerate((size_y - 1, size_y, size_y + 1)):
                for t in range(tiles):
                    up_ref[k, c, x, t : t + 1, :] = out_ref[
                        c, x, row : row + 1, t * LANES : (t + 1) * LANES
                    ]
            for k, row in enumerate((ext_y - 1, 0)):
                for t in range(tiles):
                    down_ref[k, c, x, t : t + 1, :] = out_ref[
                        c, x, row : row + 1, t * LANES : (t + 1) * LANES
                    ]
        return carry

    lax.fori_loop(0, layers, pack, 0)


def spread_out(meta, own, low, high, size_x, size_y, ext_y, depth):
    f32 = jnp.float32
    layers = size_x + 2
    tiles = depth // LANES
    return pl.pallas_call(
        functools.partial(spread_kernel, size_x, size_y, ext_y, depth),
        out_shape=(
            jax.ShapeDtypeStruct((3, layers, ext_y, depth), f32),
            jax.ShapeDtypeStruct((3, 3, layers, tiles, LANES), f32),
            jax.ShapeDtypeStruct((2, 3, layers, tiles, LANES), f32),
        ),
        in_specs=[pl.BlockSpec(memory_space=pltpu.SMEM)]
        + [pl.BlockSpec(memory_space=pltpu.VMEM)] * 3,
        out_specs=[pl.BlockSpec(memory_space=pltpu.VMEM)] * 3,
        compiler_params=pltpu.CompilerParams(vmem_limit_bytes=40 * 1024 * 1024),
        cost_estimate=pl.CostEstimate(
            flops=10_000_000_000, bytes_accessed=8_000_000, transcendentals=0
        ),
    )(meta, own, low, high)


def smoothing_kernel(
    sp_ref, up_ref, down_ref, vel_ref, visc_ref, x_low_ref, x_high_ref, y_low_ref, y_high_ref,
    out_ref, rhs_ref, field_a, field_b, up_recv, down_recv, x_send, x_recv, y_send, y_recv,
    y_last_send, y_last_recv, send_sem, recv_sem
):
    size_x, size_y, depth = visc_ref.shape
    ext_y = out_ref.shape[2]
    layers = size_x + 2
    tiles = depth // LANES
    count_x, count_y = lax.axis_size("gx"), lax.axis_size("gy")
    me_x, me_y = lax.axis_index("gx"), lax.axis_index("gy")
    x_up = (lax.rem(me_x + 1, count_x), me_y)
    x_down = (lax.rem(me_x + count_x - 1, count_x), me_y)
    y_up = (me_x, lax.rem(me_y + 1, count_y))
    y_down = (me_x, lax.rem(me_y + count_y - 1, count_y))

    barrier = pltpu.get_barrier_semaphore()
    for device in (x_up, x_down, y_up, y_down):
        pl.semaphore_signal(barrier, inc=1, device_id=device, device_id_type=MESH)
    pl.semaphore_wait(barrier, 4)

    used = [0]

    def send(source, target, device):
        sem = used[0]
        used[0] = sem + 1
        copy = pltpu.make_async_remote_copy(
            src_ref=source, dst_ref=target, send_sem=send_sem.at[sem], recv_sem=recv_sem.at[sem],
            device_id=device, device_id_type=MESH,
        )
        copy.start()
        return copy

    def row_of(ref, *index):
        return jnp.concatenate([ref[(*index, slice(t, t + 1))] for t in range(tiles)], axis=1)

    def set_row(ref, value, *index):
        for t in range(tiles):
            ref[(*index, slice(t, t + 1))] = value[:, t * LANES : (t + 1) * LANES]

    folds = (send(up_ref, up_recv, y_up), send(down_ref, down_recv, y_down))

    def build(x, carry):
        for c in range(3):
            rhs_ref[c, x, size_y:ext_y, :] = sp_ref[c, x, size_y:ext_y, :]
            rhs_ref[c, x, 0:size_y, :] = sp_ref[c, x, 0:size_y, :] + vel_ref[c, x - 1]
        return carry

    lax.fori_loop(1, size_x + 1, build, 0)
    for c in range(3):
        rhs_ref[c, 0, 0:size_y, :] = sp_ref[c, 0, 0:size_y, :] + x_low_ref[c, 0]
        rhs_ref[c, size_x + 1, 0:size_y, :] = sp_ref[c, size_x + 1, 0:size_y, :] + x_high_ref[c, 0]

    for copy in folds:
        copy.wait()

    def fold(x, carry):
        for c in range(3):
            rhs_ref[c, x, 0:1, :] += row_of(up_recv, 1, c, x)
            rhs_ref[c, x, 1:2, :] += row_of(up_recv, 2, c, x)
            rhs_ref[c, x, size_y - 1 : size_y, :] += row_of(down_recv, 0, c, x)
        return carry

    lax.fori_loop(0, layers, fold, 0)

    def fold_halo(x, carry):
        for c in range(3):
            rhs_ref[c, x, ext_y - 1 : ext_y, :] += row_of(up_recv, 0, c, x) + row_of(
                y_low_ref, c, x - 1
            )
            rhs_ref[c, x, size_y : size_y + 1, :] += row_of(down_recv, 1, c, x) + row_of(
                y_high_ref, c, x - 1
            )
        return carry

    lax.fori_loop(1, size_x + 1, fold_halo, 0)

    def update(sweep, x, low=None, high=None, edge=None):
        visc = visc_ref[x]
        scale = 1.0 / (1.0 + 6.0 * visc)
        shift = 1 if sweep == 0 else 0
        current = (rhs_ref, field_a, field_b)[sweep]
        for c in range(3):
            wide = current[c, x + shift]
            total = pltpu.roll(wide, 1, 0) + pltpu.roll(wide, ext_y - 1, 0)
            total = total + pltpu.roll(wide, 1, 1) + pltpu.roll(wide, depth - 1, 1)
            below = current[c, x + shift - 1, 0:size_y, :] if low is None else x_recv[low, c]
            above = current[c, x + shift + 1, 0:size_y, :] if high is None else x_recv[high, c]
            total = total[0:size_y] + below + above
            plane = (rhs_ref[c, x + 1, 0:size_y, :] + visc * total) * scale
            if sweep == SWEEPS - 1:
                out_ref[c, x, 0:size_y, :] = plane
                set_row(y_last_send, plane[size_y - 1 : size_y], 0, x, c)
                set_row(y_last_send, plane[0:1], 1, x, c)
                set_row(y_last_send, plane[1:2], 2, x, c)
            else:
                following = (field_a, field_b)[sweep]
                following[c, x, 0:size_y, :] = plane
                set_row(y_send, plane[size_y - 1 : size_y], sweep, 0, x, c)
                set_row(y_send, plane[0:1], sweep, 1, x, c)
                if edge is not None:
                    x_send[2 * sweep + edge, c] = plane

    def interior(sweep):
        def body(x, carry):
            update(sweep, x)
            return carry

        lax.fori_loop(1, size_x - 1, body, 0)

    def send_x(sweep):
        return (
            send(x_send.at[2 * sweep], x_recv.at[2 * sweep], x_up),
            send(x_send.at[2 * sweep + 1], x_recv.at[2 * sweep + 1], x_down),
        )

    def send_y(sweep, first, count):
        part = pl.ds(first, count)
        return (
            send(y_send.at[sweep, 0, part], y_recv.at[sweep, 0, part], y_up),
            send(y_send.at[sweep, 1, part], y_recv.at[sweep, 1, part], y_down),
        )

    def halo(sweep):
        field = (field_a, field_b)[sweep]

        def body(x, carry):
            for c in range(3):
                field[c, x, size_y : size_y + 1, :] = row_of(y_recv, sweep, 1, x, c)
                field[c, x, ext_y - 1 : ext_y, :] = row_of(y_recv, sweep, 0, x, c)
            return carry

        lax.fori_loop(0, size_x, body, 0)

    update(0, 0, edge=1)
    update(0, size_x - 1, edge=0)
    x_copies = send_x(0)
    interior(0)
    y_copies = send_y(0, 0, size_x)

    for copy in y_copies:
        copy.wait()
    halo(0)
    interior(1)
    y_copies = send_y(1, 1, size_x - 2)
    for copy in x_copies:
        copy.wait()
    update(1, 0, low=0, edge=1)
    update(1, size_x - 1, high=1, edge=0)
    x_copies = send_x(1)
    y_copies = y_copies + send_y(1, 0, 1) + send_y(1, size_x - 1, 1)
    for copy in y_copies:
        copy.wait()
    halo(1)
    interior(2)

    def send_last(first, count):
        part = pl.ds(first, count)
        return (
            send(y_last_send.at[0, part], y_last_recv.at[0, part], y_up),
            send(y_last_send.at[pl.ds(1, 2), part], y_last_recv.at[pl.ds(1, 2), part], y_down),
        )

    y_copies = send_last(1, size_x - 2)
    for copy in x_copies:
        copy.wait()
    update(2, 0, low=2)
    update(2, size_x - 1, high=3)
    y_copies = y_copies + send_last(0, 1) + send_last(size_x - 1, 1)
    for copy in y_copies:
        copy.wait()

    def halo_last(x, carry):
        for c in range(3):
            out_ref[c, x, size_y : size_y + 1, :] = row_of(y_last_recv, 1, x, c)
            out_ref[c, x, size_y + 1 : size_y + 2, :] = row_of(y_last_recv, 2, x, c)
            out_ref[c, x, size_y + 2 : ext_y - 1, :] = jnp.zeros(
                (ext_y - 3 - size_y, depth), jnp.float32
            )
            out_ref[c, x, ext_y - 1 : ext_y, :] = row_of(y_last_recv, 0, x, c)
        return carry

    lax.fori_loop(0, size_x, halo_last, 0)


def smoothed(spread, up, down, velocity, viscosity, x_low, x_high, y_low, y_high):
    size_x, size_y, depth = viscosity.shape
    layers, ext_y = spread.shape[1:3]
    tiles = depth // LANES
    f32 = jnp.float32
    copies = 24
    return pl.pallas_call(
        smoothing_kernel,
        out_shape=jax.ShapeDtypeStruct((3, size_x, ext_y, depth), f32),
        in_specs=[pl.BlockSpec(memory_space=pltpu.VMEM)] * 9,
        out_specs=pl.BlockSpec(memory_space=pltpu.VMEM),
        scratch_shapes=[
            pltpu.VMEM((3, layers, ext_y, depth), f32),
            pltpu.VMEM((3, size_x, ext_y, depth), f32),
            pltpu.VMEM((3, size_x, ext_y, depth), f32),
            pltpu.VMEM((3, 3, layers, tiles, LANES), f32),
            pltpu.VMEM((2, 3, layers, tiles, LANES), f32),
            pltpu.VMEM((4, 3, size_y, depth), f32),
            pltpu.VMEM((4, 3, size_y, depth), f32),
            pltpu.VMEM((2, 2, size_x, 3, tiles, LANES), f32),
            pltpu.VMEM((2, 2, size_x, 3, tiles, LANES), f32),
            pltpu.VMEM((3, size_x, 3, tiles, LANES), f32),
            pltpu.VMEM((3, size_x, 3, tiles, LANES), f32),
            pltpu.SemaphoreType.DMA((copies,)),
            pltpu.SemaphoreType.DMA((copies,)),
        ],
        compiler_params=pltpu.CompilerParams(
            collective_id=0, has_side_effects=True, vmem_limit_bytes=56 * 1024 * 1024
        ),
    )(spread, up, down, velocity, viscosity, x_low, x_high, y_low, y_high)


def sample_kernel(
    meta_ref, own_ref, low_ref, high_ref, field_ref, out_ref, own_out, low_out, high_out,
    field_high, field_low
):
    size_x, size_y, depth = out_ref.shape[1:]
    ext_y = field_ref.shape[2]
    tiles = depth // LANES

    def split(x, carry):
        for c in range(3):
            plane = field_ref[c, x]
            out_ref[c, x] = plane[0:size_y]
            rows = pl.ds(pl.multiple_of(x * ext_y, ext_y), ext_y)
            field_high[c, rows, :], field_low[c, rows, :] = halves(plane)
        return carry

    lax.fori_loop(0, size_x, split, 0)

    def sample(which, ref, target, x_shift, first, last):
        def chunk(j, carry):
            tile = meta_ref[which, j + 1]
            after = lax.rem(tile + 1, tiles)
            part = ref[:, lanes_of(j)]
            table_x, table_y, table_z = chunk_tables(part, tile, x_shift, FIELDS, ext_y, depth)
            z_high, z_low = halves(table_z)
            z_pair = jnp.concatenate([z_high, z_low], axis=1)
            rows = slice(first * ext_y, last * ext_y)
            for c in range(3):
                high = jnp.concatenate(
                    [field_high[c, rows, lanes_of(tile)], field_high[c, rows, lanes_of(after)]],
                    axis=1,
                )
                low = jnp.concatenate(
                    [field_low[c, rows, lanes_of(tile)], field_low[c, rows, lanes_of(after)]],
                    axis=1,
                )
                pair = jnp.dot(high, z_pair, preferred_element_type=jnp.float32)
                columns = pair[:, :LANES] + pair[:, LANES:]
                columns = columns + jnp.dot(low, z_high, preferred_element_type=jnp.float32)
                total = jnp.zeros((8, LANES), jnp.float32)
                for x in range(first, last):
                    at = (x - first) * ext_y
                    weighted = columns[at : at + ext_y] * table_y
                    summed = weighted[0:8]
                    for k in range(8, ext_y, 8):
                        summed = summed + weighted[k : k + 8]
                    total = total + summed * table_x[x : x + 1]
                target[c : c + 1, lanes_of(j)] = jnp.sum(total, axis=0, keepdims=True)
            return carry

        lax.fori_loop(0, meta_ref[which, 0], chunk, 0)

    sample(0, own_ref, own_out, -1, 0, size_x)
    sample(1, low_ref, low_out, -size_x - 1, 0, 2)
    sample(2, high_ref, high_out, size_x - 1, size_x - 1, size_x)


def sampled(meta, own, low, high, field, size_y):
    size_x, ext_y, depth = field.shape[1:]
    f32 = jnp.float32
    places = own.shape[1]
    return pl.pallas_call(
        sample_kernel,
        out_shape=(
            jax.ShapeDtypeStruct((3, size_x, size_y, depth), f32),
            jax.ShapeDtypeStruct((3, places), f32),
            jax.ShapeDtypeStruct((3, places), f32),
            jax.ShapeDtypeStruct((3, places), f32),
        ),
        in_specs=[pl.BlockSpec(memory_space=pltpu.SMEM)]
        + [pl.BlockSpec(memory_space=pltpu.VMEM)] * 4,
        out_specs=[pl.BlockSpec(memory_space=pltpu.VMEM)] * 4,
        scratch_shapes=[
            pltpu.VMEM((3, size_x * ext_y, depth), jnp.bfloat16),
            pltpu.VMEM((3, size_x * ext_y, depth), jnp.bfloat16),
        ],
        compiler_params=pltpu.CompilerParams(vmem_limit_bytes=48 * 1024 * 1024),
        cost_estimate=pl.CostEstimate(
            flops=10_000_000_000, bytes_accessed=8_000_000, transcendentals=0
        ),
    )(meta, own, low, high, field)


def ranked(onehot):
    members, kinds = onehot.shape
    group = min(128, members)
    blocks = onehot.reshape(members // group, group, kinds)
    lower = (
        lax.broadcasted_iota(jnp.int32, (group, group), 0)
        > lax.broadcasted_iota(jnp.int32, (group, group), 1)
    ).astype(jnp.float32)
    within = jnp.einsum("ij,bjd->bid", lower, blocks)
    totals = jnp.sum(blocks, axis=1)
    before = jnp.cumsum(totals, axis=0) - totals
    rank = jnp.sum((within + before[:, None, :]) * blocks, axis=-1).reshape(members)
    return rank.astype(jnp.int32), jnp.sum(totals, axis=0).astype(jnp.int32)


def onehot_of(index, kinds):
    return (index[:, None] == lax.broadcasted_iota(jnp.int32, (index.shape[0], kinds), 1)).astype(
        jnp.float32
    )


def chunk_meta(table):
    meta = jnp.concatenate([table[11, 0:1], table[10, ::LANES]])
    return meta.astype(jnp.int32)


def shards(velocity, viscosity, cells, offsets, forces, owners):
    rows_gx = lax.axis_size("gx")
    rows_gy = lax.axis_size("gy")
    devices = rows_gx * rows_gy
    markers = owners.shape[0]
    capacity = max(2, 2 * markers // devices)
    slots = capacity * devices
    size_x, size_y, depth = viscosity.shape
    ext_y = -(-(size_y + 3) // 8) * 8
    tiles = depth // LANES

    x_low = shifted(velocity[:, size_x - 1 :], "gx", 1)
    x_high = shifted(velocity[:, 0:1], "gx", -1)
    tiled = (3, size_x, tiles, LANES)
    y_low = shifted(velocity[:, :, size_y - 1].reshape(tiled), "gy", 1)
    y_high = shifted(velocity[:, :, 0].reshape(tiled), "gy", -1)

    owner = owners[:, 0]
    rank, _ = ranked(onehot_of(owner, devices))
    slot = owner * capacity + rank
    payload = jnp.concatenate(
        [cells.astype(jnp.float32), offsets, forces, jnp.ones((1, markers), jnp.float32)], axis=0
    )
    outgoing = jnp.zeros((10, slots), jnp.float32).at[:, slot].set(payload, unique_indices=True)
    received = exchanged(outgoing, capacity, 1)

    valid = received[9] > 0.5
    start = received[2].astype(jnp.int32) - 1
    bins = jnp.where(start < 0, start + depth, start) // LANES
    bins = jnp.where(valid, bins, tiles)
    chunks = slots // LANES + tiles
    places = chunks * LANES
    rank, totals = ranked(onehot_of(bins, tiles))
    needed = (totals + (LANES - 1)) // LANES
    ends = jnp.cumsum(needed)
    first = ends - needed
    shift = jnp.sum(jnp.where(bins[:, None] == jnp.arange(tiles)[None, :], first[None, :], 0), axis=1)
    spot = jnp.where(valid, shift * LANES + rank, places)
    tile_of = jnp.sum(jnp.arange(chunks)[:, None] >= ends[None, :], axis=1)
    tile_of = jnp.minimum(tile_of, tiles - 1).astype(jnp.float32)
    own = jnp.zeros((10, places), jnp.float32).at[:, spot].set(
        received, mode="drop", unique_indices=True
    )
    own = jnp.concatenate(
        [
            own,
            jnp.repeat(tile_of, LANES)[None],
            jnp.full((1, places), ends[-1].astype(jnp.float32)),
            jnp.zeros((4, places), jnp.float32),
        ],
        axis=0,
    )
    low = shifted(own, "gx", 1)
    high = shifted(own, "gx", -1)
    meta = jnp.stack([chunk_meta(own), chunk_meta(low), chunk_meta(high)])

    spread, up, down = spread_out(meta, own, low, high, size_x, size_y, ext_y, depth)
    field = smoothed(spread, up, down, velocity, viscosity, x_low, x_high, y_low, y_high)
    new_velocity, values, low_values, high_values = sampled(meta, own, low, high, field, size_y)
    values = values + shifted(low_values, "gx", -1) + shifted(high_values, "gx", 1)
    back = values[:, jnp.minimum(spot, places - 1)]
    back = jnp.where(valid[None], back, 0.0)
    returned = exchanged(back, capacity, 2)
    return (new_velocity, returned[:, slot])


def solution(mesh):
    in_specs = (
        P(None, "gx", "gy", None),
        P("gx", "gy", None),
        P(None, ("gx", "gy")),
        P(None, ("gx", "gy")),
        P(None, ("gx", "gy")),
        P(("gx", "gy"), None),
    )
    out_specs = (P(None, "gx", "gy", None), P(None, ("gx", "gy")))
    return jax.shard_map(shards, mesh=mesh, in_specs=in_specs, out_specs=out_specs, check_vma=False)
```

```python
import functools

import jax
import jax.numpy as jnp
from jax import lax
from jax.experimental import pallas as pl
from jax.experimental.pallas import tpu as pltpu
from jax.sharding import PartitionSpec as P


MESH = pl.DeviceIdType.MESH

SWEEPS = 3
LANES = 128


def shifted(block, axis, step):
    count = lax.axis_size(axis)
    return lax.ppermute(block, axis, [(i, (i + step) % count) for i in range(count)])


def kernel_weights(frac):
    root = jnp.sqrt(1.0 + 4.0 * frac - 4.0 * frac * frac)
    return (
        (3.0 - 2.0 * frac - root) * 0.125,
        (3.0 - 2.0 * frac + root) * 0.125,
        (1.0 + 2.0 * frac + root) * 0.125,
        (1.0 + 2.0 * frac - root) * 0.125,
    )


def exchange_kernel(out_ref, in_ref, send_sem, recv_sem):
    count_x, count_y = lax.axis_size("gx"), lax.axis_size("gy")
    devices = count_x * count_y
    me = lax.axis_index("gx") * count_y + lax.axis_index("gy")

    def place(index):
        return (lax.div(index, count_y), lax.rem(index, count_y))

    barrier = pltpu.get_barrier_semaphore()

    def greet(k, carry):
        pl.semaphore_signal(
            barrier, inc=1, device_id=place(lax.rem(me + k, devices)), device_id_type=MESH
        )
        return carry

    lax.fori_loop(1, devices, greet, 0)
    pl.semaphore_wait(barrier, devices - 1)

    def copy(k, source, target):
        return pltpu.make_async_remote_copy(
            src_ref=out_ref.at[target], dst_ref=in_ref.at[source],
            send_sem=send_sem.at[k], recv_sem=recv_sem.at[k],
            device_id=place(target), device_id_type=MESH,
        )

    def begin(k, carry):
        copy(k, me, lax.rem(me + k, devices)).start()
        return carry

    def finish(k, carry):
        target = lax.rem(me + k, devices)
        source = lax.rem(me + devices - k, devices)
        copy(k, me, target).wait_send()
        copy(k, source, target).wait_recv()
        return carry

    lax.fori_loop(1, devices, begin, 0)
    in_ref[me] = out_ref[me]
    lax.fori_loop(1, devices, finish, 0)


def exchanged(values, count, collective_id):
    devices = lax.axis_size("gx") * lax.axis_size("gy")
    rows = values.shape[0]
    tile = 8 * LANES
    sized = -(-rows * count // tile) * tile
    flat = values.reshape(rows, devices, count).transpose(1, 0, 2).reshape(devices, rows * count)
    flat = jnp.pad(flat, ((0, 0), (0, sized - rows * count)))
    flat = flat.reshape(devices, sized // LANES, LANES)
    received = pl.pallas_call(
        exchange_kernel,
        out_shape=jax.ShapeDtypeStruct(flat.shape, jnp.float32),
        in_specs=[pl.BlockSpec(memory_space=pltpu.VMEM)],
        out_specs=pl.BlockSpec(memory_space=pltpu.VMEM),
        scratch_shapes=[pltpu.SemaphoreType.DMA((devices,)), pltpu.SemaphoreType.DMA((devices,))],
        compiler_params=pltpu.CompilerParams(collective_id=collective_id, has_side_effects=True),
    )(flat)
    received = received.reshape(devices, sized)[:, : rows * count].reshape(devices, rows, count)
    return received.transpose(1, 0, 2).reshape(rows, devices * count)


def tent(first, weights, length, wrap=0):
    rows = lax.broadcasted_iota(jnp.int32, (length, LANES), 0)
    table = jnp.zeros((length, LANES), jnp.float32)
    for j in range(4):
        target = first + j
        if wrap:
            target = jnp.where(target < 0, target + wrap, target)
            target = jnp.where(target >= wrap, target - wrap, target)
        table = table + jnp.where(rows == target, weights[j], 0.0)
    return table


def halves(value):
    high = value.astype(jnp.bfloat16)
    low = (value - high.astype(jnp.float32)).astype(jnp.bfloat16)
    return high, low


def chunk_tables(part, tile, x_shift, layers, ext_y, depth):
    cells = part[0:3].astype(jnp.int32)
    table_x = tent(cells[0:1] + x_shift, kernel_weights(part[3:4]), layers)
    table_y = tent(cells[1:2] - 1, kernel_weights(part[4:5]), ext_y, ext_y)
    start = cells[2:3] - 1
    start = jnp.where(start < 0, start + depth, start) - tile * LANES
    table_z = tent(start, kernel_weights(part[5:6]), 2 * LANES)
    return table_x, table_y, table_z


def chunk_count(ref):
    return jnp.max(ref[11:12, 0:LANES]).astype(jnp.int32)


def note_tiles(tables, tile_ref):
    for k, ref in enumerate(tables):
        for j in range(ref.shape[1] // LANES):
            tile = jnp.max(ref[10:11, j * LANES : (j + 1) * LANES])
            tile_ref[k, j] = tile.astype(jnp.int32)


def lanes_of(tile):
    return pl.ds(pl.multiple_of(tile * LANES, LANES), LANES)


def transposed_dot(left, right):
    return lax.dot_general(
        left, right, (((1,), (1,)), ((), ())), preferred_element_type=jnp.float32
    )


def padded(count):
    return -(-count // 8) * 8


def spread_kernel(shifts, together, *refs):
    tables, outs, tile_ref = refs[: len(shifts)], refs[len(shifts) : -1], refs[-1]

    def clear(out_ref):
        def body(i, carry):
            for c in range(3):
                out_ref[c, i] = jnp.zeros(out_ref.shape[2:], jnp.float32)
            return carry

        lax.fori_loop(0, out_ref.shape[1], body, 0)

    for out_ref in outs:
        clear(out_ref)
    note_tiles(tables, tile_ref)

    def product(which, j):
        ref, out_ref = tables[which], outs[which]
        layers, ext_y, depth = out_ref.shape[1:]
        part = ref[:, lanes_of(j)]
        table_x, table_y, table_z = chunk_tables(
            part, tile_ref[which, j], shifts[which], padded(layers), ext_y, depth
        )
        z_high, z_low = halves(table_z)
        z_pair = jnp.concatenate([z_high, z_high], axis=1)
        planes = []
        for c in range(3):
            pushed = table_x * part[6 + c : 7 + c]
            planes += [pushed[x : x + 1] * table_y for x in range(layers)]
        high, low = halves(jnp.concatenate(planes, axis=0))
        total = transposed_dot(jnp.concatenate([high, low], axis=1), z_pair)
        return total + transposed_dot(high, z_low)

    def add(which, j, total):
        out_ref = outs[which]
        layers, ext_y, depth = out_ref.shape[1:]
        shape = (3, layers, ext_y, LANES)
        tile = tile_ref[which, j]
        after = lax.rem(tile + 1, depth // LANES)
        out_ref[:, :, :, lanes_of(tile)] += total[:, :LANES].reshape(shape)
        out_ref[:, :, :, lanes_of(after)] += total[:, LANES:].reshape(shape)

    def chunk(j, carry):
        kinds = range(len(tables))
        steps = [(which, together * j + k) for which in kinds for k in range(together)]
        totals = [product(*step) for step in steps]
        for step, total in zip(steps, totals):
            add(*step, total)
        return carry

    count = chunk_count(tables[0])
    for ref in tables[1:]:
        count = jnp.maximum(count, chunk_count(ref))
    lax.fori_loop(0, lax.div(count + (together - 1), together), chunk, 0)


def spread_out(tables, shifts, layers, together, ext_y, depth, cost):
    chunks = tables[0].shape[1] // LANES
    return pl.pallas_call(
        functools.partial(spread_kernel, shifts, together),
        out_shape=[
            jax.ShapeDtypeStruct((3, count, ext_y, depth), jnp.float32) for count in layers
        ],
        in_specs=[pl.BlockSpec(memory_space=pltpu.VMEM)] * len(tables),
        out_specs=[pl.BlockSpec(memory_space=pltpu.VMEM)] * len(tables),
        scratch_shapes=[pltpu.SMEM((len(tables), chunks), jnp.int32)],
        compiler_params=pltpu.CompilerParams(vmem_limit_bytes=24 * 1024 * 1024),
        cost_estimate=pl.CostEstimate(flops=cost, bytes_accessed=1_000_000, transcendentals=0),
    )(*tables)


def smoothing_kernel(
    own_ref, below_ref, above_ref, vel_hbm, visc_hbm, vel_low, vel_high, out_ref, vel_ref,
    visc_ref, rhs_ref, field_a, field_b, fold_send, fold_recv, x_send, x_recv, y_send, y_recv,
    last_send, last_recv, load_sem, send_sem, recv_sem
):
    size_x, size_y, depth = visc_hbm.shape
    ext_y = out_ref.shape[2]
    layers = size_x + 2
    tiles = depth // LANES
    count_x, count_y = lax.axis_size("gx"), lax.axis_size("gy")
    me_x, me_y = lax.axis_index("gx"), lax.axis_index("gy")
    x_up = (lax.rem(me_x + 1, count_x), me_y)
    x_down = (lax.rem(me_x + count_x - 1, count_x), me_y)
    y_up = (me_x, lax.rem(me_y + 1, count_y))
    y_down = (me_x, lax.rem(me_y + count_y - 1, count_y))

    loads = [
        pltpu.make_async_copy(source, target, load_sem.at[k])
        for k, (source, target) in enumerate(
            (
                (vel_low, vel_ref.at[:, 0:1]),
                (vel_high, vel_ref.at[:, size_x + 1 :]),
                (vel_hbm, vel_ref.at[:, 1 : size_x + 1]),
                (visc_hbm, visc_ref),
            )
        )
    ]
    for copy in loads:
        copy.start()

    barrier = pltpu.get_barrier_semaphore()
    for device in (x_up, x_down, y_up, y_down):
        pl.semaphore_signal(barrier, inc=1, device_id=device, device_id_type=MESH)
    pl.semaphore_wait(barrier, 4)

    used = [0]

    def send(source, target, device):
        sem = used[0]
        used[0] = sem + 1
        copy = pltpu.make_async_remote_copy(
            src_ref=source, dst_ref=target, send_sem=send_sem.at[sem], recv_sem=recv_sem.at[sem],
            device_id=device, device_id_type=MESH,
        )
        copy.start()
        return copy

    def wait(copies):
        for copy in copies:
            copy.wait()

    def row_of(ref, *index):
        return jnp.concatenate([ref[(*index, slice(t, t + 1))] for t in range(tiles)], axis=1)

    def set_row(ref, value, *index):
        for t in range(tiles):
            ref[(*index, slice(t, t + 1))] = value[:, t * LANES : (t + 1) * LANES]

    def build(x, beside=None, at=0):
        for c in range(3):
            plane = own_ref[c, x]
            if beside is not None:
                plane = plane + beside[c, x - at]
            inner = plane[0:size_y] + vel_ref[c, x]
            rhs_ref[c, x, size_y:ext_y, :] = plane[size_y:ext_y]
            rhs_ref[c, x, 0:size_y, :] = inner
            set_row(fold_send, inner[size_y - 1 : size_y], x, 0, c)
            set_row(fold_send, plane[size_y : size_y + 1], x, 1, c)
            set_row(fold_send, plane[size_y + 1 : size_y + 2], x, 2, c)
            set_row(fold_send, plane[ext_y - 1 : ext_y], x, 3, c)
            set_row(fold_send, inner[0:1], x, 4, c)

    def send_fold(first, count):
        part = pl.ds(first, count)
        return (
            send(fold_send.at[part, 0:3], fold_recv.at[part, 0:3], y_up),
            send(fold_send.at[part, 3:5], fold_recv.at[part, 3:5], y_down),
        )

    def fold(x, carry):
        for c in range(3):
            rhs_ref[c, x, 0:1, :] += row_of(fold_recv, x, 1, c)
            rhs_ref[c, x, 1:2, :] += row_of(fold_recv, x, 2, c)
            rhs_ref[c, x, size_y - 1 : size_y, :] += row_of(fold_recv, x, 3, c)
            rhs_ref[c, x, ext_y - 1 : ext_y, :] += row_of(fold_recv, x, 0, c)
            rhs_ref[c, x, size_y : size_y + 1, :] += row_of(fold_recv, x, 4, c)
        return carry

    below, above = below_ref.shape[1], above_ref.shape[1]

    def lower(x, carry):
        build(x, below_ref, 0)
        return carry

    def middle(x, carry):
        build(x)
        return carry

    def upper(x, carry):
        build(x, above_ref, layers - above)
        return carry

    wait(loads)
    lax.fori_loop(0, below, lower, 0)
    low_fold = send_fold(0, 3)
    lax.fori_loop(layers - above, layers, upper, 0)
    middle(layers - 3, 0)
    high_fold = send_fold(layers - 3, 3)
    lax.fori_loop(3, layers - 3, middle, 0)
    middle_fold = send_fold(3, layers - 6)

    def update(sweep, x, low=None, high=None, edge=None):
        visc = visc_ref[x]
        scale = 1.0 / (1.0 + 6.0 * visc)
        shift = 1 if sweep == 0 else 0
        current = (rhs_ref, field_a, field_b)[sweep]
        for c in range(3):
            wide = current[c, x + shift]
            total = pltpu.roll(wide, 1, 0) + pltpu.roll(wide, ext_y - 1, 0)
            total = total + pltpu.roll(wide, 1, 1) + pltpu.roll(wide, depth - 1, 1)
            before = current[c, x + shift - 1, 0:size_y, :] if low is None else x_recv[low, c]
            behind = current[c, x + shift + 1, 0:size_y, :] if high is None else x_recv[high, c]
            total = total[0:size_y] + before + behind
            plane = (rhs_ref[c, x + 1, 0:size_y, :] + visc * total) * scale
            if sweep == SWEEPS - 1:
                out_ref[c, x, 0:size_y, :] = plane
                set_row(last_send, plane[size_y - 1 : size_y], 0, x, c)
                set_row(last_send, plane[0:1], 1, x, c)
                set_row(last_send, plane[1:2], 2, x, c)
            else:
                (field_a, field_b)[sweep][c, x, 0:size_y, :] = plane
                set_row(y_send, plane[size_y - 1 : size_y], sweep, 0, x, c)
                set_row(y_send, plane[0:1], sweep, 1, x, c)
                if edge is not None:
                    x_send[2 * sweep + edge, c] = plane

    def interior(sweep):
        def body(x, carry):
            update(sweep, x)
            return carry

        lax.fori_loop(1, size_x - 1, body, 0)

    def send_x(sweep, way):
        slot = 2 * sweep + way
        return send(x_send.at[slot], x_recv.at[slot], (x_up, x_down)[way])

    def send_y(sweep, first, count):
        part = pl.ds(first, count)
        return (
            send(y_send.at[sweep, 0, part], y_recv.at[sweep, 0, part], y_up),
            send(y_send.at[sweep, 1, part], y_recv.at[sweep, 1, part], y_down),
        )

    def send_last(first, count):
        part = pl.ds(first, count)
        return (
            send(last_send.at[0, part], last_recv.at[0, part], y_up),
            send(last_send.at[1:3, part], last_recv.at[1:3, part], y_down),
        )

    def halo(sweep):
        field = (field_a, field_b)[sweep]

        def body(x, carry):
            for c in range(3):
                field[c, x, size_y : size_y + 1, :] = row_of(y_recv, sweep, 1, x, c)
                field[c, x, ext_y - 1 : ext_y, :] = row_of(y_recv, sweep, 0, x, c)
            return carry

        lax.fori_loop(0, size_x, body, 0)

    def halo_last(x, carry):
        for c in range(3):
            out_ref[c, x, size_y : size_y + 1, :] = row_of(last_recv, 1, x, c)
            out_ref[c, x, size_y + 1 : size_y + 2, :] = row_of(last_recv, 2, x, c)
            out_ref[c, x, size_y + 2 : ext_y - 1, :] = jnp.zeros(
                (ext_y - 3 - size_y, depth), jnp.float32
            )
            out_ref[c, x, ext_y - 1 : ext_y, :] = row_of(last_recv, 0, x, c)
        return carry

    wait(low_fold)
    lax.fori_loop(0, 3, fold, 0)
    update(0, 0, edge=1)
    x_copies = (send_x(0, 1),)
    wait(high_fold)
    lax.fori_loop(layers - 3, layers, fold, 0)
    update(0, size_x - 1, edge=0)
    x_copies = x_copies + (send_x(0, 0),)
    wait(middle_fold)
    lax.fori_loop(3, layers - 3, fold, 0)
    interior(0)
    y_copies = send_y(0, 0, size_x)
    wait(y_copies)
    halo(0)
    interior(1)
    y_copies = send_y(1, 1, size_x - 2)
    wait(x_copies)
    update(1, 0, low=0, edge=1)
    x_copies = (send_x(1, 1),)
    update(1, size_x - 1, high=1, edge=0)
    x_copies = x_copies + (send_x(1, 0),)
    y_copies = y_copies + send_y(1, 0, 1) + send_y(1, size_x - 1, 1)
    wait(y_copies)
    halo(1)
    interior(2)
    y_copies = send_last(1, size_x - 2)
    wait(y_copies)
    lax.fori_loop(1, size_x - 1, halo_last, 0)
    wait(x_copies)
    update(2, 0, low=2)
    y_copies = send_last(0, 1)
    update(2, size_x - 1, high=3)
    y_copies = y_copies + send_last(size_x - 1, 1)
    wait(y_copies)
    halo_last(0, 0)
    halo_last(size_x - 1, 0)


def smoothed(own, below, above, velocity, viscosity, vel_low, vel_high):
    size_x, size_y, depth = viscosity.shape
    ext_y = own.shape[2]
    layers = size_x + 2
    tiles = depth // LANES
    f32 = jnp.float32
    vmem, hbm = pl.BlockSpec(memory_space=pltpu.VMEM), pl.BlockSpec(memory_space=pl.ANY)
    return pl.pallas_call(
        smoothing_kernel,
        out_shape=jax.ShapeDtypeStruct((3, size_x, ext_y, depth), f32),
        in_specs=[vmem] * 3 + [hbm] * 4,
        out_specs=vmem,
        scratch_shapes=[
            pltpu.VMEM((3, layers, size_y, depth), f32),
            pltpu.VMEM((size_x, size_y, depth), f32),
            pltpu.VMEM((3, layers, ext_y, depth), f32),
            pltpu.VMEM((3, size_x, ext_y, depth), f32),
            pltpu.VMEM((3, size_x, ext_y, depth), f32),
            pltpu.VMEM((layers, 5, 3, tiles, LANES), f32),
            pltpu.VMEM((layers, 5, 3, tiles, LANES), f32),
            pltpu.VMEM((4, 3, size_y, depth), f32),
            pltpu.VMEM((4, 3, size_y, depth), f32),
            pltpu.VMEM((2, 2, size_x, 3, tiles, LANES), f32),
            pltpu.VMEM((2, 2, size_x, 3, tiles, LANES), f32),
            pltpu.VMEM((3, size_x, 3, tiles, LANES), f32),
            pltpu.VMEM((3, size_x, 3, tiles, LANES), f32),
            pltpu.SemaphoreType.DMA((4,)),
            pltpu.SemaphoreType.DMA((24,)),
            pltpu.SemaphoreType.DMA((24,)),
        ],
        compiler_params=pltpu.CompilerParams(
            collective_id=0, has_side_effects=True, vmem_limit_bytes=36 * 1024 * 1024
        ),
    )(own, below, above, velocity, viscosity, vel_low, vel_high)


def sample_chunk(ref, tile, j, target, x_shift, high_of, low_of):
    layers, ext_y, depth = high_of.shape[1:]
    after = lax.rem(tile + 1, depth // LANES)
    table_x, table_y, table_z = chunk_tables(
        ref[:, lanes_of(j)], tile, x_shift, padded(layers), ext_y, depth
    )
    z_high, z_low = halves(table_z)
    z_pair = jnp.concatenate([z_high, z_low], axis=1)

    def window(ref):
        rows = (3 * layers * ext_y, LANES)
        return jnp.concatenate(
            [
                ref[:, :, :, lanes_of(tile)].reshape(rows),
                ref[:, :, :, lanes_of(after)].reshape(rows),
            ],
            axis=1,
        )

    pair = jnp.dot(window(high_of), z_pair, preferred_element_type=jnp.float32)
    columns = pair[:, :LANES] + pair[:, LANES:]
    columns = columns + jnp.dot(window(low_of), z_high, preferred_element_type=jnp.float32)
    for c in range(3):
        total = jnp.zeros((8, LANES), jnp.float32)
        for x in range(layers):
            at = (c * layers + x) * ext_y
            weighted = columns[at : at + ext_y] * table_y
            summed = weighted[0:8]
            for k in range(8, ext_y, 8):
                summed = summed + weighted[k : k + 8]
            total = total + summed * table_x[x : x + 1]
        target[c : c + 1, lanes_of(j)] = jnp.sum(total, axis=0, keepdims=True)


def sample_kernel(table_ref, field_ref, vel_ref, out_ref, field_high, field_low, tile_ref):
    size_x, size_y = vel_ref.shape[1:3]

    def split(x, carry):
        for c in range(3):
            plane = field_ref[c, x]
            vel_ref[c, x] = plane[0:size_y]
            field_high[c, x], field_low[c, x] = halves(plane)
        return carry

    lax.fori_loop(0, size_x, split, 0)
    note_tiles([table_ref], tile_ref)

    def chunk(i, carry):
        for j in (2 * i, 2 * i + 1):
            sample_chunk(table_ref, tile_ref[0, j], j, out_ref, -1, field_high, field_low)
        return carry

    lax.fori_loop(0, lax.div(chunk_count(table_ref) + 1, 2), chunk, 0)


def sampled(table, field, size_y):
    size_x, ext_y, depth = field.shape[1:]
    f32 = jnp.float32
    vmem = pl.BlockSpec(memory_space=pltpu.VMEM)
    return pl.pallas_call(
        sample_kernel,
        out_shape=(
            jax.ShapeDtypeStruct((3, size_x, size_y, depth), f32),
            jax.ShapeDtypeStruct((3, table.shape[1]), f32),
        ),
        in_specs=[vmem] * 2,
        out_specs=[vmem] * 2,
        scratch_shapes=[pltpu.VMEM((3, size_x, ext_y, depth), jnp.bfloat16)] * 2
        + [pltpu.SMEM((1, table.shape[1] // LANES), jnp.int32)],
        compiler_params=pltpu.CompilerParams(vmem_limit_bytes=28 * 1024 * 1024),
        cost_estimate=pl.CostEstimate(
            flops=10_000_000_000, bytes_accessed=1_000_000, transcendentals=0
        ),
    )(table, field)


def sample_beside_kernel(
    low_ref, high_ref, field_ref, low_out, high_out, first_high, first_low, last_high, last_low,
    tile_ref
):
    size_x = field_ref.shape[1]
    for c in range(3):
        for x in range(2):
            first_high[c, x], first_low[c, x] = halves(field_ref[c, x])
        last_high[c, 0], last_low[c, 0] = halves(field_ref[c, size_x - 1])
    note_tiles([low_ref, high_ref], tile_ref)

    def chunk(j, carry):
        sample_chunk(
            low_ref, tile_ref[0, j], j, low_out, -size_x - 1, first_high, first_low
        )
        sample_chunk(high_ref, tile_ref[1, j], j, high_out, 0, last_high, last_low)
        return carry

    lax.fori_loop(0, jnp.maximum(chunk_count(low_ref), chunk_count(high_ref)), chunk, 0)


def sampled_beside(low, high, field):
    ext_y, depth = field.shape[2:]
    vmem = pl.BlockSpec(memory_space=pltpu.VMEM)
    return pl.pallas_call(
        sample_beside_kernel,
        out_shape=[jax.ShapeDtypeStruct((3, low.shape[1]), jnp.float32)] * 2,
        in_specs=[vmem] * 3,
        out_specs=[vmem] * 2,
        scratch_shapes=[pltpu.VMEM((3, 2, ext_y, depth), jnp.bfloat16)] * 2
        + [pltpu.VMEM((3, 1, ext_y, depth), jnp.bfloat16)] * 2
        + [pltpu.SMEM((2, low.shape[1] // LANES), jnp.int32)],
        compiler_params=pltpu.CompilerParams(vmem_limit_bytes=16 * 1024 * 1024),
        cost_estimate=pl.CostEstimate(
            flops=2_000_000_000, bytes_accessed=1_000_000, transcendentals=0
        ),
    )(low, high, field)


def ranked(onehot):
    members, kinds = onehot.shape
    group = min(128, members)
    blocks = onehot.reshape(members // group, group, kinds)
    lower = (
        lax.broadcasted_iota(jnp.int32, (group, group), 0)
        > lax.broadcasted_iota(jnp.int32, (group, group), 1)
    ).astype(jnp.float32)
    within = jnp.einsum("ij,bjd->bid", lower, blocks)
    totals = jnp.sum(blocks, axis=1)
    before = jnp.cumsum(totals, axis=0) - totals
    rank = jnp.sum((within + before[:, None, :]) * blocks, axis=-1).reshape(members)
    return rank.astype(jnp.int32), jnp.sum(totals, axis=0).astype(jnp.int32)


def onehot_of(index, kinds):
    return (index[:, None] == lax.broadcasted_iota(jnp.int32, (index.shape[0], kinds), 1)).astype(
        jnp.float32
    )


def stepped(velocity, viscosity, cells, offsets, forces, owners):
    rows_gx = lax.axis_size("gx")
    rows_gy = lax.axis_size("gy")
    devices = rows_gx * rows_gy
    markers = owners.shape[0]
    capacity = max(2, 2 * markers // devices)
    slots = capacity * devices
    size_x, size_y, depth = viscosity.shape
    ext_y = -(-(size_y + 3) // 8) * 8
    tiles = depth // LANES

    owner = owners[:, 0]
    rank, _ = ranked(onehot_of(owner, devices))
    slot = owner * capacity + rank
    payload = jnp.concatenate(
        [cells.astype(jnp.float32), offsets, forces, jnp.ones((1, markers), jnp.float32)], axis=0
    )
    outgoing = jnp.zeros((10, slots), jnp.float32).at[:, slot].set(payload, unique_indices=True)
    received = exchanged(outgoing, capacity, 1)
    edges = (velocity[:, size_x - 1 :], velocity[:, 0:1])
    received, edges = lax.optimization_barrier((received, edges))
    vel_low = shifted(edges[0], "gx", 1)
    vel_high = shifted(edges[1], "gx", -1)

    valid = received[9] > 0.5
    start = received[2].astype(jnp.int32) - 1
    bins = jnp.where(start < 0, start + depth, start) // LANES
    bins = jnp.where(valid, bins, tiles)
    chunks = -(-(slots // LANES + tiles) // 2) * 2
    places = chunks * LANES
    rank, totals = ranked(onehot_of(bins, tiles))
    needed = (totals + (LANES - 1)) // LANES
    ends = jnp.cumsum(needed)
    first = ends - needed
    shift = jnp.sum(jnp.where(bins[:, None] == jnp.arange(tiles)[None, :], first[None, :], 0), axis=1)
    spot = jnp.where(valid, shift * LANES + rank, places)
    count = jnp.full((slots,), ends[-1].astype(jnp.float32))
    sorting = jnp.concatenate([received, jnp.stack([bins.astype(jnp.float32), count])], axis=0)
    own = jnp.zeros((12, places), jnp.float32).at[:, spot].set(
        sorting, mode="drop", unique_indices=True
    )
    low = shifted(own, "gx", 1)
    high = shifted(own, "gx", -1)

    (spread,) = spread_out([own], (0,), (size_x + 2,), 2, ext_y, depth, 10_000_000_000)
    below, above = spread_out(
        [low, high], (-size_x, 0), (3, 2), 1, ext_y, depth, 2_000_000_000,
    )
    field = smoothed(spread, below, above, velocity, viscosity, vel_low, vel_high)
    low_values, high_values = sampled_beside(low, high, field)
    low_values = shifted(low_values, "gx", -1)
    high_values = shifted(high_values, "gx", 1)
    new_velocity, values = sampled(own, field, size_y)
    values = values + low_values + high_values
    back = values[:, jnp.minimum(spot, places - 1)]
    back = jnp.where(valid[None], back, 0.0)
    returned = exchanged(back, capacity, 2)
    return (new_velocity, returned[:, slot])


def solution(mesh):
    in_specs = (
        P(None, "gx", "gy", None),
        P("gx", "gy", None),
        P(None, ("gx", "gy")),
        P(None, ("gx", "gy")),
        P(None, ("gx", "gy")),
        P(("gx", "gy"), None),
    )
    out_specs = (P(None, "gx", "gy", None), P(None, ("gx", "gy")))
    return jax.shard_map(stepped, mesh=mesh, in_specs=in_specs, out_specs=out_specs, check_vma=False)
```

```python
import functools

import jax
import jax.numpy as jnp
from jax import lax
from jax.experimental import pallas as pl
from jax.experimental.pallas import tpu as pltpu
from jax.sharding import PartitionSpec as P


MESH = pl.DeviceIdType.MESH

SWEEPS = 3
LANES = 128
SPREAD_BELOW = 3
SPREAD_ABOVE = 2


def shifted(block, axis, step):
    count = lax.axis_size(axis)
    return lax.ppermute(block, axis, [(i, (i + step) % count) for i in range(count)])


def kernel_weights(frac):
    root = jnp.sqrt(1.0 + 4.0 * frac - 4.0 * frac * frac)
    return (
        (3.0 - 2.0 * frac - root) * 0.125,
        (3.0 - 2.0 * frac + root) * 0.125,
        (1.0 + 2.0 * frac + root) * 0.125,
        (1.0 + 2.0 * frac - root) * 0.125,
    )


def thirds(value):
    high = value.astype(jnp.bfloat16)
    rest = value - high.astype(jnp.float32)
    middle = rest.astype(jnp.bfloat16)
    low = (rest - middle.astype(jnp.float32)).astype(jnp.bfloat16)
    return jnp.concatenate([high, middle, low], axis=0)


def rejoined(parts, rows):
    return (parts[0:rows] + parts[rows : 2 * rows]) + parts[2 * rows : 3 * rows]


def flags(match):
    return jnp.where(match, 1.0, 0.0).astype(jnp.bfloat16)


class Exchange:
    def __init__(self, out_ref, in_ref, send_sem, recv_sem):
        self.out_ref, self.in_ref = out_ref, in_ref
        self.send_sem, self.recv_sem = send_sem, recv_sem
        self.count_y = lax.axis_size("gy")
        self.devices = lax.axis_size("gx") * self.count_y
        self.me = lax.axis_index("gx") * self.count_y + lax.axis_index("gy")
        self.barrier = pltpu.get_barrier_semaphore()

    def place(self, index):
        return (lax.div(index, self.count_y), lax.rem(index, self.count_y))

    def other(self, k):
        return lax.rem(self.me + k, self.devices)

    def greet(self):
        def body(k, carry):
            pl.semaphore_signal(
                self.barrier, inc=1, device_id=self.place(self.other(k)), device_id_type=MESH
            )
            return carry

        lax.fori_loop(1, self.devices, body, 0)

    def copy(self, k, source, target):
        return pltpu.make_async_remote_copy(
            src_ref=self.out_ref.at[target], dst_ref=self.in_ref.at[source],
            send_sem=self.send_sem.at[k], recv_sem=self.recv_sem.at[k],
            device_id=self.place(target), device_id_type=MESH,
        )

    def start(self):
        pl.semaphore_wait(self.barrier, self.devices - 1)

        def body(k, carry):
            self.copy(k, self.me, self.other(k)).start()
            return carry

        lax.fori_loop(1, self.devices, body, 0)
        self.in_ref[self.me] = self.out_ref[self.me]

    def finish(self):
        def body(k, carry):
            source = lax.rem(self.me + self.devices - k, self.devices)
            self.copy(k, self.me, self.other(k)).wait_send()
            self.copy(k, source, self.me).wait_recv()
            return carry

        lax.fori_loop(1, self.devices, body, 0)


def turned(value, amount):
    return value if amount % LANES == 0 else pltpu.roll(value, amount % LANES, 1)


def lane_between(first, last):
    lane = lax.broadcasted_iota(jnp.int32, (8, LANES), 1)
    return (lane >= first) & (lane < last)


def put_tiles(out_ref, block, first, second, capacity):
    for k in range(LANES // capacity):
        tile = jnp.where(lane_between(0, capacity), turned(first, -k * capacity), 0.0)
        if second is not None:
            tile = jnp.where(
                lane_between(capacity, 2 * capacity), turned(second, capacity - k * capacity), tile
            )
        out_ref[block * (LANES // capacity) + k] = tile


def block_of(in_ref, block, capacity, half):
    total = jnp.zeros((8, LANES), jnp.float32)
    for k in range(LANES // capacity):
        tile = in_ref[block * (LANES // capacity) + k]
        total = jnp.where(
            lane_between(k * capacity, (k + 1) * capacity),
            turned(tile, (k - half) * capacity),
            total,
        )
    return total


def route_kernel(
    capacity, owner_hbm, cells_hbm, offsets_hbm, forces_hbm, slot_ref, table_ref, out_ref, in_ref,
    owner_ref, cells_ref, offsets_ref, forces_ref, load_sem, send_sem, recv_sem
):
    f32 = jnp.float32
    loads = [
        pltpu.make_async_copy(source, target, load_sem.at[k])
        for k, (source, target) in enumerate(
            (
                (owner_hbm, owner_ref), (cells_hbm, cells_ref), (offsets_hbm, offsets_ref),
                (forces_hbm, forces_ref),
            )
        )
    ]
    for copy in loads:
        copy.start()
    exchange = Exchange(out_ref, in_ref, send_sem, recv_sem)
    exchange.greet()
    for copy in loads:
        copy.wait()
    markers = owner_ref.shape[1]
    slots = capacity * exchange.devices
    owner = owner_ref[...].astype(f32)
    lanes = lax.broadcasted_iota(jnp.int32, (LANES, markers), 1)
    rows = lax.broadcasted_iota(jnp.int32, (LANES, markers), 0)
    before = jnp.zeros((8, markers), f32)
    for j in range(0, markers, LANES):
        group = jnp.broadcast_to(owner[:, j : j + LANES], (LANES, LANES))
        column = jnp.transpose(group)
        column = jnp.concatenate([column] * (markers // LANES), axis=1)
        same = jnp.where((column == owner) & (rows + j < lanes), 1.0, 0.0)
        for k in range(0, LANES, 8):
            before = before + same[k : k + 8]
    slot = (owner * capacity + jnp.sum(before, axis=0, keepdims=True)).astype(jnp.int32)
    slot_ref[...] = slot
    payload = jnp.concatenate(
        [
            cells_ref[...].astype(f32), offsets_ref[...], forces_ref[...],
            jnp.ones((1, markers), f32), jnp.zeros((6, markers), f32),
        ],
        axis=0,
    )
    split = thirds(payload)
    wide = 2 * LANES

    def pack(i, carry):
        place = lax.broadcasted_iota(jnp.int32, (wide, markers), 0) + i * wide
        sent = rejoined(transposed_dot(split, flags(place == slot)), 16)
        for k in range(2):
            part = sent[:, k * LANES : (k + 1) * LANES]
            put_tiles(out_ref, 2 * i + k, part[0:8], part[8:16], capacity)
        return carry

    lax.fori_loop(0, slots // wide, pack, 0)
    exchange.start()
    exchange.finish()

    def unpack(i, carry):
        table_ref[0:8, lanes_of(i)] = block_of(in_ref, i, capacity, 0)
        table_ref[8:16, lanes_of(i)] = block_of(in_ref, i, capacity, 1)
        return carry

    lax.fori_loop(0, slots // LANES, unpack, 0)


def routed(owner, cells, offsets, forces, capacity):
    devices = lax.axis_size("gx") * lax.axis_size("gy")
    markers = owner.shape[1]
    f32 = jnp.float32
    vmem = pl.BlockSpec(memory_space=pltpu.VMEM)
    return pl.pallas_call(
        functools.partial(route_kernel, capacity),
        out_shape=(
            jax.ShapeDtypeStruct((1, markers), jnp.int32),
            jax.ShapeDtypeStruct((16, devices * capacity), f32),
        ),
        in_specs=[pl.BlockSpec(memory_space=pltpu.HBM)] * 4,
        out_specs=[vmem] * 2,
        scratch_shapes=[pltpu.VMEM((devices, 8, LANES), f32)] * 2
        + [pltpu.VMEM((1, markers), jnp.int32), pltpu.VMEM((3, markers), jnp.int32)]
        + [pltpu.VMEM((3, markers), f32)] * 2
        + [pltpu.SemaphoreType.DMA((4,))]
        + [pltpu.SemaphoreType.DMA((devices,))] * 2,
        compiler_params=pltpu.CompilerParams(
            collective_id=1, has_side_effects=True, vmem_limit_bytes=24 * 1024 * 1024
        ),
    )(owner, cells, offsets, forces)


def sort_kernel(depth, size_x, received_ref, place_ref, table_ref):
    f32 = jnp.float32
    slots = received_ref.shape[1]
    tiles = depth // LANES
    blocks = slots // LANES
    valid = received_ref[9:10] > 0.5
    start = received_ref[2:3].astype(jnp.int32) - 1
    bins = jnp.where(start < 0, start + depth, start)
    bins = jnp.where(valid, lax.shift_right_logical(bins, LANES.bit_length() - 1), tiles)
    cell = received_ref[0:1].astype(jnp.int32)
    edge = valid & ((cell < SPREAD_ABOVE) | (cell >= size_x - SPREAD_BELOW))
    kinds = lax.broadcasted_iota(jnp.int32, (2 * tiles, slots), 0)
    member = jnp.where(kinds == 2 * bins + jnp.where(edge, 0, 1), 1.0, 0.0)
    stacked = jnp.concatenate(
        [member[:, b * LANES : (b + 1) * LANES] for b in range(blocks)], axis=0
    ).astype(jnp.bfloat16)
    above = lax.broadcasted_iota(jnp.int32, (LANES, LANES), 0) < lax.broadcasted_iota(
        jnp.int32, (LANES, LANES), 1
    )
    within = jnp.dot(stacked, flags(above), preferred_element_type=f32)
    sums = jnp.dot(stacked, jnp.ones((LANES, LANES), jnp.bfloat16), preferred_element_type=f32)
    ranks, run = [], jnp.zeros((2 * tiles, LANES), f32)
    for b in range(blocks):
        ranks.append(within[2 * b * tiles : 2 * (b + 1) * tiles] + run)
        run = run + sums[2 * b * tiles : 2 * (b + 1) * tiles]
    run = run.astype(jnp.int32)
    firsts, total = [], jnp.zeros((1, LANES), jnp.int32)
    lane = lax.broadcasted_iota(jnp.int32, (1, LANES), 1)
    tile_of, order, edge_total = jnp.zeros_like(total), jnp.zeros_like(total), total

    def chunks_for(amount):
        return lax.shift_right_logical(amount + (LANES - 1), LANES.bit_length() - 1)

    for k in range(tiles):
        edges, others = run[2 * k : 2 * k + 1], run[2 * k + 1 : 2 * k + 2]
        firsts += [total * LANES, total * LANES + edges]
        edge_chunks = chunks_for(edges)
        inside = (lane >= edge_total) & (lane < edge_total + edge_chunks)
        order = jnp.where(inside, total + lane - edge_total, order)
        edge_total = edge_total + edge_chunks
        total = total + chunks_for(edges + others)
        tile_of = tile_of + jnp.where(lane >= total, 1, 0)
    tile_of = jnp.minimum(tile_of, tiles - 1)
    order = jnp.where(lane >= edge_total, table_ref.shape[1] // LANES - 1, order)
    first = jnp.concatenate(firsts, axis=0).astype(f32)
    spots = jnp.concatenate(
        [
            jnp.sum(
                member[:, b * LANES : (b + 1) * LANES] * (ranks[b] + first), axis=0, keepdims=True
            )
            for b in range(blocks)
        ],
        axis=1,
    )
    place = jnp.where(valid, spots.astype(jnp.int32), -1)
    place_ref[...] = place
    count = jnp.max(total.astype(f32)).astype(jnp.int32)
    payload = jnp.concatenate(
        [
            received_ref[0:9], jnp.zeros((7, slots), f32),
        ],
        axis=0,
    )
    split = thirds(payload)
    table_ref[...] = jnp.zeros(table_ref.shape, f32)
    wide = 2 * LANES

    def gather(i, carry):
        spot = lax.broadcasted_iota(jnp.int32, (wide, slots), 0) + i * wide
        sorted_part = rejoined(transposed_dot(split, flags(spot == place)), 16)
        table_ref[:, pl.ds(pl.multiple_of(i * wide, wide), wide)] = sorted_part
        return carry

    lax.fori_loop(0, lax.div(count + 1, 2), gather, 0)
    for row, value in enumerate((tile_of, order, edge_total, total)):
        table_ref[12 + row : 13 + row, 0:LANES] = value.astype(f32)


def sorted_table(received, places, depth, size_x):
    vmem = pl.BlockSpec(memory_space=pltpu.VMEM)
    return pl.pallas_call(
        functools.partial(sort_kernel, depth, size_x),
        out_shape=(
            jax.ShapeDtypeStruct((1, received.shape[1]), jnp.int32),
            jax.ShapeDtypeStruct((16, places), jnp.float32),
        ),
        in_specs=[vmem],
        out_specs=[vmem] * 2,
        compiler_params=pltpu.CompilerParams(vmem_limit_bytes=16 * 1024 * 1024),
        cost_estimate=pl.CostEstimate(
            flops=3_000_000_000, bytes_accessed=1_000_000, transcendentals=0
        ),
    )(received)


def return_kernel(
    capacity, slot_ref, place_ref, own_ref, low_ref, high_ref, out_values_ref, out_ref, in_ref,
    marks_ref, back_ref, send_sem, recv_sem
):
    f32 = jnp.float32
    exchange = Exchange(out_ref, in_ref, send_sem, recv_sem)
    exchange.greet()
    slots, markers = marks_ref.shape
    places = own_ref.shape[1]
    wide = 2 * LANES
    place = place_ref[...]
    blank = jnp.zeros((5, wide), f32)

    def unsort(i, total):
        part = pl.ds(pl.multiple_of(i * wide, wide), wide)
        values = own_ref[:, part] + low_ref[:, part] + high_ref[:, part]
        split = thirds(jnp.concatenate([values, blank], axis=0))
        spot = lax.broadcasted_iota(jnp.int32, (wide, slots), 0) + i * wide
        return total + jnp.dot(split, flags(spot == place), preferred_element_type=f32)

    total = lax.fori_loop(0, places // wide, unsort, jnp.zeros((24, slots), f32))
    back_ref[...] = rejoined(total, 8)

    def pack(i, carry):
        put_tiles(out_ref, i, back_ref[:, lanes_of(i)], None, capacity)
        return carry

    lax.fori_loop(0, slots // LANES, pack, 0)
    exchange.start()
    slot = slot_ref[...]

    def mark(i, carry):
        rows = pl.ds(pl.multiple_of(i * LANES, LANES), LANES)
        here = lax.broadcasted_iota(jnp.int32, (LANES, markers), 0) + i * LANES
        marks_ref[rows, :] = flags(here == slot)
        return carry

    lax.fori_loop(0, slots // LANES, mark, 0)
    exchange.finish()

    def unpack(i, carry):
        back_ref[:, lanes_of(i)] = block_of(in_ref, i, capacity, 0)
        return carry

    lax.fori_loop(0, slots // LANES, unpack, 0)
    parts = jnp.dot(thirds(back_ref[...]), marks_ref[...], preferred_element_type=f32)
    out_values_ref[...] = rejoined(parts, 8)[0:3]


def given_back(slot, place, values, low_values, high_values, capacity):
    devices = lax.axis_size("gx") * lax.axis_size("gy")
    markers, slots = slot.shape[1], place.shape[1]
    f32 = jnp.float32
    vmem = pl.BlockSpec(memory_space=pltpu.VMEM)
    return pl.pallas_call(
        functools.partial(return_kernel, capacity),
        out_shape=jax.ShapeDtypeStruct((3, markers), f32),
        in_specs=[vmem] * 5,
        out_specs=vmem,
        scratch_shapes=[pltpu.VMEM((devices, 8, LANES), f32)] * 2
        + [pltpu.VMEM((slots, markers), jnp.bfloat16), pltpu.VMEM((8, slots), f32)]
        + [pltpu.SemaphoreType.DMA((devices,))] * 2,
        compiler_params=pltpu.CompilerParams(
            collective_id=2, has_side_effects=True, vmem_limit_bytes=24 * 1024 * 1024
        ),
    )(slot, place, values, low_values, high_values)


def tent(first, weights, length, wrap=0):
    rows = lax.broadcasted_iota(jnp.int32, (length, LANES), 0)
    table = jnp.zeros((length, LANES), jnp.float32)
    for j in range(4):
        target = first + j
        if wrap:
            target = jnp.where(target < 0, target + wrap, target)
            target = jnp.where(target >= wrap, target - wrap, target)
        table = table + jnp.where(rows == target, weights[j], 0.0)
    return table


def halves(value):
    high = value.astype(jnp.bfloat16)
    low = (value - high.astype(jnp.float32)).astype(jnp.bfloat16)
    return high, low


def chunk_tables(part, tile, x_shift, layers, ext_y, depth, marker_rows):
    cells = part[0:3].astype(jnp.int32)
    table_x = tent(cells[0:1] + x_shift, kernel_weights(part[3:4]), layers)
    table_y = tent(cells[1:2] - 1, kernel_weights(part[4:5]), ext_y, ext_y)
    start = cells[2:3] - 1
    start = jnp.where(start < 0, start + depth, start) - tile * LANES
    weights = kernel_weights(part[5:6])
    if not marker_rows:
        return table_x, table_y, tent(start, weights, 2 * LANES)
    packed = jnp.concatenate(
        [start.astype(jnp.float32), *weights, jnp.zeros((3, LANES), jnp.float32)], axis=0
    )
    columns = jnp.transpose(packed)
    where = lax.broadcasted_iota(jnp.int32, (LANES, 2 * LANES), 1).astype(jnp.float32)
    where = where - columns[:, 0:1]
    table_z = jnp.zeros((LANES, 2 * LANES), jnp.float32)
    for k in range(4):
        table_z = jnp.where(where == float(k), columns[:, k + 1 : k + 2], table_z)
    return table_x, table_y, table_z


def chunk_notes(tables, note_ref, note_sem):
    copies = [
        pltpu.make_async_copy(ref.at[8:16, 0:LANES], note_ref.at[k], note_sem.at[k])
        for k, ref in enumerate(tables)
    ]
    for copy in copies:
        copy.start()
    return copies


def note(note_ref, which, row, at):
    return note_ref[which, row, at].astype(jnp.int32)


def note_scratch(tables):
    return [pltpu.SMEM((tables, 8, LANES), jnp.float32), pltpu.SemaphoreType.DMA((tables,))]


def lanes_of(tile):
    return pl.ds(pl.multiple_of(tile * LANES, LANES), LANES)


def transposed_dot(left, right):
    return lax.dot_general(
        left, right, (((1,), (1,)), ((), ())), preferred_element_type=jnp.float32
    )


def padded(count):
    return -(-count // 8) * 8


def spread_kernel(shifts, together, *refs):
    tables, outs = refs[: len(shifts)], refs[len(shifts) : -2]
    note_ref, note_sem = refs[-2:]
    beside = len(tables) > 1
    copies = chunk_notes(tables, note_ref, note_sem)

    def clear(out_ref):
        def body(i, carry):
            for c in range(3):
                out_ref[c, i] = jnp.zeros(out_ref.shape[2:], jnp.float32)
            return carry

        lax.fori_loop(0, out_ref.shape[1], body, 0)

    for out_ref in outs:
        clear(out_ref)
    for copy in copies:
        copy.wait()

    def product(which, j):
        ref, out_ref = tables[which], outs[which]
        layers, ext_y, depth = out_ref.shape[1:]
        part = ref[:, lanes_of(j)]
        table_x, table_y, table_z = chunk_tables(
            part, note(note_ref, which, 4, j), shifts[which], padded(layers), ext_y, depth, True
        )
        z_high, z_low = halves(table_z)
        z_pair = jnp.concatenate([z_high, z_high], axis=0)
        planes = []
        for c in range(3):
            pushed = table_x * part[6 + c : 7 + c]
            planes += [pushed[x : x + 1] * table_y for x in range(layers)]
        high, low = halves(jnp.concatenate(planes, axis=0))
        total = jnp.dot(
            jnp.concatenate([high, low], axis=1), z_pair, preferred_element_type=jnp.float32
        )
        return total + jnp.dot(high, z_low, preferred_element_type=jnp.float32)

    def add(which, j, total):
        out_ref = outs[which]
        layers, ext_y, depth = out_ref.shape[1:]
        shape = (3, layers, ext_y, LANES)
        tile = note(note_ref, which, 4, j)
        after = lax.rem(tile + 1, depth // LANES)
        out_ref[:, :, :, lanes_of(tile)] += total[:, :LANES].reshape(shape)
        out_ref[:, :, :, lanes_of(after)] += total[:, LANES:].reshape(shape)

    def chunk(j, carry):
        kinds = range(len(tables))
        steps = [
            (which, note(note_ref, which, 5, j) if beside else together * j + k)
            for which in kinds
            for k in range(together)
        ]
        totals = [product(*step) for step in steps]
        for step, total in zip(steps, totals):
            add(*step, total)
        return carry

    counts = [note(note_ref, which, 6 if beside else 7, 0) for which in range(len(tables))]
    count = functools.reduce(jnp.maximum, counts)
    lax.fori_loop(0, lax.div(count + (together - 1), together), chunk, 0)


def spread_out(tables, shifts, layers, together, ext_y, depth, cost):
    return pl.pallas_call(
        functools.partial(spread_kernel, shifts, together),
        out_shape=[
            jax.ShapeDtypeStruct((3, count, ext_y, depth), jnp.float32) for count in layers
        ],
        in_specs=[pl.BlockSpec(memory_space=pltpu.VMEM)] * len(tables),
        out_specs=[pl.BlockSpec(memory_space=pltpu.VMEM)] * len(tables),
        scratch_shapes=note_scratch(len(tables)),
        compiler_params=pltpu.CompilerParams(vmem_limit_bytes=24 * 1024 * 1024),
        cost_estimate=pl.CostEstimate(flops=cost, bytes_accessed=1_000_000, transcendentals=0),
    )(*tables)


def smoothing_kernel(
    own_ref, below_ref, above_ref, vel_hbm, visc_hbm, vel_low, vel_high, out_ref, vel_ref,
    visc_ref, rhs_ref, field_a, field_b, fold_send, fold_recv, x_send, x_recv, y_send, y_recv,
    last_send, last_recv, load_sem, send_sem, recv_sem
):
    size_x, size_y, depth = visc_hbm.shape
    ext_y = out_ref.shape[2]
    layers = size_x + 2
    tiles = depth // LANES
    count_x, count_y = lax.axis_size("gx"), lax.axis_size("gy")
    me_x, me_y = lax.axis_index("gx"), lax.axis_index("gy")
    x_up = (lax.rem(me_x + 1, count_x), me_y)
    x_down = (lax.rem(me_x + count_x - 1, count_x), me_y)
    y_up = (me_x, lax.rem(me_y + 1, count_y))
    y_down = (me_x, lax.rem(me_y + count_y - 1, count_y))

    loads = [
        pltpu.make_async_copy(source, target, load_sem.at[k])
        for k, (source, target) in enumerate(
            (
                (vel_low, vel_ref.at[:, 0:1]),
                (vel_high, vel_ref.at[:, size_x + 1 :]),
                (vel_hbm, vel_ref.at[:, 1 : size_x + 1]),
                (visc_hbm, visc_ref),
            )
        )
    ]
    for copy in loads:
        copy.start()

    barrier = pltpu.get_barrier_semaphore()
    for device in (x_up, x_down, y_up, y_down):
        pl.semaphore_signal(barrier, inc=1, device_id=device, device_id_type=MESH)
    pl.semaphore_wait(barrier, 4)

    used = [0]

    def send(source, target, device):
        sem = used[0]
        used[0] = sem + 1
        copy = pltpu.make_async_remote_copy(
            src_ref=source, dst_ref=target, send_sem=send_sem.at[sem], recv_sem=recv_sem.at[sem],
            device_id=device, device_id_type=MESH,
        )
        copy.start()
        return copy

    def wait(copies):
        for copy in copies:
            copy.wait()

    def row_of(ref, *index):
        return jnp.concatenate([ref[(*index, slice(t, t + 1))] for t in range(tiles)], axis=1)

    def set_row(ref, value, *index):
        for t in range(tiles):
            ref[(*index, slice(t, t + 1))] = value[:, t * LANES : (t + 1) * LANES]

    def build(x, beside=None, at=0):
        for c in range(3):
            plane = own_ref[c, x]
            if beside is not None:
                plane = plane + beside[c, x - at]
            inner = plane[0:size_y] + vel_ref[c, x]
            rhs_ref[c, x, size_y:ext_y, :] = plane[size_y:ext_y]
            rhs_ref[c, x, 0:size_y, :] = inner
            set_row(fold_send, inner[size_y - 1 : size_y], x, 0, c)
            set_row(fold_send, plane[size_y : size_y + 1], x, 1, c)
            set_row(fold_send, plane[size_y + 1 : size_y + 2], x, 2, c)
            set_row(fold_send, plane[ext_y - 1 : ext_y], x, 3, c)
            set_row(fold_send, inner[0:1], x, 4, c)

    def send_fold(first, count):
        part = pl.ds(first, count)
        return (
            send(fold_send.at[part, 0:3], fold_recv.at[part, 0:3], y_up),
            send(fold_send.at[part, 3:5], fold_recv.at[part, 3:5], y_down),
        )

    def fold(x, carry):
        for c in range(3):
            rhs_ref[c, x, 0:1, :] += row_of(fold_recv, x, 1, c)
            rhs_ref[c, x, 1:2, :] += row_of(fold_recv, x, 2, c)
            rhs_ref[c, x, size_y - 1 : size_y, :] += row_of(fold_recv, x, 3, c)
            rhs_ref[c, x, ext_y - 1 : ext_y, :] += row_of(fold_recv, x, 0, c)
            rhs_ref[c, x, size_y : size_y + 1, :] += row_of(fold_recv, x, 4, c)
        return carry

    below, above = below_ref.shape[1], above_ref.shape[1]

    def lower(x, carry):
        build(x, below_ref, 0)
        return carry

    def middle(x, carry):
        build(x)
        return carry

    def upper(x, carry):
        build(x, above_ref, layers - above)
        return carry

    wait(loads)
    lax.fori_loop(0, below, lower, 0)
    low_fold = send_fold(0, 3)
    lax.fori_loop(layers - above, layers, upper, 0)
    middle(layers - 3, 0)
    high_fold = send_fold(layers - 3, 3)
    lax.fori_loop(3, layers - 3, middle, 0)
    middle_fold = send_fold(3, layers - 6)

    def update(sweep, x, low=None, high=None, edge=None):
        visc = visc_ref[x]
        scale = 1.0 / (1.0 + 6.0 * visc)
        shift = 1 if sweep == 0 else 0
        current = (rhs_ref, field_a, field_b)[sweep]
        for c in range(3):
            wide = current[c, x + shift]
            total = pltpu.roll(wide, 1, 0) + pltpu.roll(wide, ext_y - 1, 0)
            total = total + pltpu.roll(wide, 1, 1) + pltpu.roll(wide, depth - 1, 1)
            before = current[c, x + shift - 1, 0:size_y, :] if low is None else x_recv[low, c]
            behind = current[c, x + shift + 1, 0:size_y, :] if high is None else x_recv[high, c]
            total = total[0:size_y] + before + behind
            plane = (rhs_ref[c, x + 1, 0:size_y, :] + visc * total) * scale
            if sweep == SWEEPS - 1:
                out_ref[c, x, 0:size_y, :] = plane
                set_row(last_send, plane[size_y - 1 : size_y], 0, x, c)
                set_row(last_send, plane[0:1], 1, x, c)
                set_row(last_send, plane[1:2], 2, x, c)
            else:
                (field_a, field_b)[sweep][c, x, 0:size_y, :] = plane
                set_row(y_send, plane[size_y - 1 : size_y], sweep, 0, x, c)
                set_row(y_send, plane[0:1], sweep, 1, x, c)
                if edge is not None:
                    x_send[2 * sweep + edge, c] = plane

    def interior(sweep):
        def body(x, carry):
            update(sweep, x)
            return carry

        lax.fori_loop(1, size_x - 1, body, 0)

    def send_x(sweep, way):
        slot = 2 * sweep + way
        return send(x_send.at[slot], x_recv.at[slot], (x_up, x_down)[way])

    def send_y(sweep, first, count):
        part = pl.ds(first, count)
        return (
            send(y_send.at[sweep, 0, part], y_recv.at[sweep, 0, part], y_up),
            send(y_send.at[sweep, 1, part], y_recv.at[sweep, 1, part], y_down),
        )

    def send_last(first, count):
        part = pl.ds(first, count)
        return (
            send(last_send.at[0, part], last_recv.at[0, part], y_up),
            send(last_send.at[1:3, part], last_recv.at[1:3, part], y_down),
        )

    def halo(sweep):
        field = (field_a, field_b)[sweep]

        def body(x, carry):
            for c in range(3):
                field[c, x, size_y : size_y + 1, :] = row_of(y_recv, sweep, 1, x, c)
                field[c, x, ext_y - 1 : ext_y, :] = row_of(y_recv, sweep, 0, x, c)
            return carry

        lax.fori_loop(0, size_x, body, 0)

    def halo_last(x, carry):
        for c in range(3):
            out_ref[c, x, size_y : size_y + 1, :] = row_of(last_recv, 1, x, c)
            out_ref[c, x, size_y + 1 : size_y + 2, :] = row_of(last_recv, 2, x, c)
            out_ref[c, x, size_y + 2 : ext_y - 1, :] = jnp.zeros(
                (ext_y - 3 - size_y, depth), jnp.float32
            )
            out_ref[c, x, ext_y - 1 : ext_y, :] = row_of(last_recv, 0, x, c)
        return carry

    wait(low_fold)
    lax.fori_loop(0, 3, fold, 0)
    update(0, 0, edge=1)
    x_copies = (send_x(0, 1),)
    wait(high_fold)
    lax.fori_loop(layers - 3, layers, fold, 0)
    update(0, size_x - 1, edge=0)
    x_copies = x_copies + (send_x(0, 0),)
    wait(middle_fold)
    lax.fori_loop(3, layers - 3, fold, 0)
    interior(0)
    y_copies = send_y(0, 0, size_x)
    wait(y_copies)
    halo(0)
    interior(1)
    y_copies = send_y(1, 1, size_x - 2)
    wait(x_copies)
    update(1, 0, low=0, edge=1)
    x_copies = (send_x(1, 1),)
    update(1, size_x - 1, high=1, edge=0)
    x_copies = x_copies + (send_x(1, 0),)
    y_copies = y_copies + send_y(1, 0, 1) + send_y(1, size_x - 1, 1)
    wait(y_copies)
    halo(1)
    interior(2)
    y_copies = send_last(1, size_x - 2)
    wait(y_copies)
    lax.fori_loop(1, size_x - 1, halo_last, 0)
    wait(x_copies)
    update(2, 0, low=2)
    y_copies = send_last(0, 1)
    update(2, size_x - 1, high=3)
    y_copies = y_copies + send_last(size_x - 1, 1)
    wait(y_copies)
    halo_last(0, 0)
    halo_last(size_x - 1, 0)


def smoothed(own, below, above, velocity, viscosity, vel_low, vel_high):
    size_x, size_y, depth = viscosity.shape
    ext_y = own.shape[2]
    layers = size_x + 2
    tiles = depth // LANES
    f32 = jnp.float32
    vmem, hbm = pl.BlockSpec(memory_space=pltpu.VMEM), pl.BlockSpec(memory_space=pltpu.HBM)
    return pl.pallas_call(
        smoothing_kernel,
        out_shape=jax.ShapeDtypeStruct((3, size_x, ext_y, depth), f32),
        in_specs=[vmem] * 3 + [hbm] * 4,
        out_specs=vmem,
        scratch_shapes=[
            pltpu.VMEM((3, layers, size_y, depth), f32),
            pltpu.VMEM((size_x, size_y, depth), f32),
            pltpu.VMEM((3, layers, ext_y, depth), f32),
            pltpu.VMEM((3, size_x, ext_y, depth), f32),
            pltpu.VMEM((3, size_x, ext_y, depth), f32),
            pltpu.VMEM((layers, 5, 3, tiles, LANES), f32),
            pltpu.VMEM((layers, 5, 3, tiles, LANES), f32),
            pltpu.VMEM((4, 3, size_y, depth), f32),
            pltpu.VMEM((4, 3, size_y, depth), f32),
            pltpu.VMEM((2, 2, size_x, 3, tiles, LANES), f32),
            pltpu.VMEM((2, 2, size_x, 3, tiles, LANES), f32),
            pltpu.VMEM((3, size_x, 3, tiles, LANES), f32),
            pltpu.VMEM((3, size_x, 3, tiles, LANES), f32),
            pltpu.SemaphoreType.DMA((4,)),
            pltpu.SemaphoreType.DMA((24,)),
            pltpu.SemaphoreType.DMA((24,)),
        ],
        compiler_params=pltpu.CompilerParams(
            collective_id=0, has_side_effects=True, vmem_limit_bytes=32 * 1024 * 1024
        ),
    )(own, below, above, velocity, viscosity, vel_low, vel_high)


def sample_chunk(ref, tile, j, target, x_shift, high_of, low_of):
    layers, ext_y, depth = high_of.shape[1:]
    after = lax.rem(tile + 1, depth // LANES)
    table_x, table_y, table_z = chunk_tables(
        ref[:, lanes_of(j)], tile, x_shift, padded(layers), ext_y, depth, False
    )
    z_high, z_low = halves(table_z)
    z_pair = jnp.concatenate([z_high, z_low], axis=1)

    def window(ref):
        rows = (3 * layers * ext_y, LANES)
        return jnp.concatenate(
            [
                ref[:, :, :, lanes_of(tile)].reshape(rows),
                ref[:, :, :, lanes_of(after)].reshape(rows),
            ],
            axis=1,
        )

    pair = jnp.dot(window(high_of), z_pair, preferred_element_type=jnp.float32)
    columns = pair[:, :LANES] + pair[:, LANES:]
    columns = columns + jnp.dot(window(low_of), z_high, preferred_element_type=jnp.float32)
    for c in range(3):
        total = jnp.zeros((8, LANES), jnp.float32)
        for x in range(layers):
            at = (c * layers + x) * ext_y
            weighted = columns[at : at + ext_y] * table_y
            summed = weighted[0:8]
            for k in range(8, ext_y, 8):
                summed = summed + weighted[k : k + 8]
            total = total + summed * table_x[x : x + 1]
        target[c : c + 1, lanes_of(j)] = jnp.sum(total, axis=0, keepdims=True)


def sample_kernel(table_ref, field_ref, vel_ref, out_ref, field_high, field_low, note_ref, note_sem):
    size_x, size_y = vel_ref.shape[1:3]
    copies = chunk_notes([table_ref], note_ref, note_sem)

    def split(x, carry):
        for c in range(3):
            plane = field_ref[c, x]
            vel_ref[c, x] = plane[0:size_y]
            field_high[c, x], field_low[c, x] = halves(plane)
        return carry

    lax.fori_loop(0, size_x, split, 0)
    copies[0].wait()
    out_ref[...] = jnp.zeros(out_ref.shape, jnp.float32)

    def chunk(i, carry):
        for j in (2 * i, 2 * i + 1):
            tile = note(note_ref, 0, 4, j)
            sample_chunk(table_ref, tile, j, out_ref, -1, field_high, field_low)
        return carry

    lax.fori_loop(0, lax.div(note(note_ref, 0, 7, 0) + 1, 2), chunk, 0)


def sampled(table, field, size_y):
    size_x, ext_y, depth = field.shape[1:]
    f32 = jnp.float32
    vmem = pl.BlockSpec(memory_space=pltpu.VMEM)
    return pl.pallas_call(
        sample_kernel,
        out_shape=(
            jax.ShapeDtypeStruct((3, size_x, size_y, depth), f32),
            jax.ShapeDtypeStruct((3, table.shape[1]), f32),
        ),
        in_specs=[vmem] * 2,
        out_specs=[vmem] * 2,
        scratch_shapes=[pltpu.VMEM((3, size_x, ext_y, depth), jnp.bfloat16)] * 2
        + note_scratch(1),
        compiler_params=pltpu.CompilerParams(vmem_limit_bytes=28 * 1024 * 1024),
        cost_estimate=pl.CostEstimate(
            flops=10_000_000_000, bytes_accessed=1_000_000, transcendentals=0
        ),
    )(table, field)


def sample_beside_kernel(
    low_ref, high_ref, field_ref, low_out, high_out, first_high, first_low, last_high, last_low,
    note_ref, note_sem
):
    size_x = field_ref.shape[1]
    copies = chunk_notes([low_ref, high_ref], note_ref, note_sem)
    for c in range(3):
        for x in range(2):
            first_high[c, x], first_low[c, x] = halves(field_ref[c, x])
        last_high[c, 0], last_low[c, 0] = halves(field_ref[c, size_x - 1])
    for copy in copies:
        copy.wait()
    low_out[...] = jnp.zeros(low_out.shape, jnp.float32)
    high_out[...] = jnp.zeros(high_out.shape, jnp.float32)

    def chunk(i, carry):
        j = note(note_ref, 0, 5, i)
        tile = note(note_ref, 0, 4, j)
        sample_chunk(low_ref, tile, j, low_out, -size_x - 1, first_high, first_low)
        j = note(note_ref, 1, 5, i)
        tile = note(note_ref, 1, 4, j)
        sample_chunk(high_ref, tile, j, high_out, 0, last_high, last_low)
        return carry

    count = jnp.maximum(note(note_ref, 0, 6, 0), note(note_ref, 1, 6, 0))
    lax.fori_loop(0, count, chunk, 0)


def sampled_beside(low, high, field):
    ext_y, depth = field.shape[2:]
    vmem = pl.BlockSpec(memory_space=pltpu.VMEM)
    return pl.pallas_call(
        sample_beside_kernel,
        out_shape=[jax.ShapeDtypeStruct((3, low.shape[1]), jnp.float32)] * 2,
        in_specs=[vmem] * 3,
        out_specs=[vmem] * 2,
        scratch_shapes=[pltpu.VMEM((3, 2, ext_y, depth), jnp.bfloat16)] * 2
        + [pltpu.VMEM((3, 1, ext_y, depth), jnp.bfloat16)] * 2
        + note_scratch(2),
        compiler_params=pltpu.CompilerParams(vmem_limit_bytes=16 * 1024 * 1024),
        cost_estimate=pl.CostEstimate(
            flops=2_000_000_000, bytes_accessed=1_000_000, transcendentals=0
        ),
    )(low, high, field)


def stepped(velocity, viscosity, cells, offsets, forces, owners):
    rows_gx = lax.axis_size("gx")
    rows_gy = lax.axis_size("gy")
    devices = rows_gx * rows_gy
    markers = owners.shape[0]
    capacity = max(2, 2 * markers // devices)
    slots = capacity * devices
    size_x, size_y, depth = viscosity.shape
    ext_y = -(-(size_y + 3) // 8) * 8
    tiles = depth // LANES

    slot, received = routed(owners.reshape(1, markers), cells, offsets, forces, capacity)
    received, edge = lax.optimization_barrier((received, velocity[:, size_x - 1 :]))
    vel_low = shifted(edge, "gx", 1)
    chunks = -(-(slots // LANES + tiles) // 2) * 2
    place, own = sorted_table(received, chunks * LANES, depth, size_x)
    own, edge = lax.optimization_barrier((own, velocity[:, 0:1]))
    low = shifted(own, "gx", 1)
    high = shifted(own, "gx", -1)
    vel_high = shifted(edge, "gx", -1)
    (spread,) = spread_out([own], (0,), (size_x + 2,), 2, ext_y, depth, 10_000_000_000)
    below, above = spread_out(
        [low, high], (-size_x, 0), (SPREAD_BELOW, SPREAD_ABOVE), 1, ext_y, depth,
        2_000_000_000,
    )
    field = smoothed(spread, below, above, velocity, viscosity, vel_low, vel_high)
    low_values, high_values = sampled_beside(low, high, field)
    low_values = shifted(low_values, "gx", -1)
    high_values = shifted(high_values, "gx", 1)
    new_velocity, values = sampled(own, field, size_y)
    marker_velocity = given_back(slot, place, values, low_values, high_values, capacity)
    return (new_velocity, marker_velocity)


def solution(mesh):
    in_specs = (
        P(None, "gx", "gy", None),
        P("gx", "gy", None),
        P(None, ("gx", "gy")),
        P(None, ("gx", "gy")),
        P(None, ("gx", "gy")),
        P(("gx", "gy"), None),
    )
    out_specs = (P(None, "gx", "gy", None), P(None, ("gx", "gy")))
    return jax.shard_map(stepped, mesh=mesh, in_specs=in_specs, out_specs=out_specs, check_vma=False)
```

```python
import functools

import jax
import jax.numpy as jnp
from jax import lax
from jax.experimental import pallas as pl
from jax.experimental.pallas import tpu as pltpu
from jax.sharding import PartitionSpec as P


MESH = pl.DeviceIdType.MESH

SWEEPS = 3
LANES = 128
SPREAD_BELOW = 3
SPREAD_ABOVE = 2


def shifted(block, axis, step):
    count = lax.axis_size(axis)
    return lax.ppermute(block, axis, [(i, (i + step) % count) for i in range(count)])


def kernel_weights(frac):
    root = jnp.sqrt(1.0 + 4.0 * frac - 4.0 * frac * frac)
    return (
        (3.0 - 2.0 * frac - root) * 0.125,
        (3.0 - 2.0 * frac + root) * 0.125,
        (1.0 + 2.0 * frac + root) * 0.125,
        (1.0 + 2.0 * frac - root) * 0.125,
    )


def thirds(value):
    high = value.astype(jnp.bfloat16)
    rest = value - high.astype(jnp.float32)
    middle = rest.astype(jnp.bfloat16)
    low = (rest - middle.astype(jnp.float32)).astype(jnp.bfloat16)
    return jnp.concatenate([high, middle, low], axis=0)


def rejoined(parts, rows):
    return (parts[0:rows] + parts[rows : 2 * rows]) + parts[2 * rows : 3 * rows]


def flags(match):
    return jnp.where(match, 1.0, 0.0).astype(jnp.bfloat16)


class Exchange:
    def __init__(self, out_ref, in_ref, send_sem, recv_sem):
        self.out_ref, self.in_ref = out_ref, in_ref
        self.send_sem, self.recv_sem = send_sem, recv_sem
        self.count_y = lax.axis_size("gy")
        self.devices = lax.axis_size("gx") * self.count_y
        self.me = lax.axis_index("gx") * self.count_y + lax.axis_index("gy")
        self.barrier = pltpu.get_barrier_semaphore()

    def place(self, index):
        return (lax.div(index, self.count_y), lax.rem(index, self.count_y))

    def other(self, k):
        return lax.rem(self.me + k, self.devices)

    def greet(self):
        def body(k, carry):
            pl.semaphore_signal(
                self.barrier, inc=1, device_id=self.place(self.other(k)), device_id_type=MESH
            )
            return carry

        lax.fori_loop(1, self.devices, body, 0)

    def copy(self, k, source, target):
        return pltpu.make_async_remote_copy(
            src_ref=self.out_ref.at[target], dst_ref=self.in_ref.at[source],
            send_sem=self.send_sem.at[k], recv_sem=self.recv_sem.at[k],
            device_id=self.place(target), device_id_type=MESH,
        )

    def start(self):
        pl.semaphore_wait(self.barrier, self.devices - 1)

        def body(k, carry):
            self.copy(k, self.me, self.other(k)).start()
            return carry

        lax.fori_loop(1, self.devices, body, 0)
        self.in_ref[self.me] = self.out_ref[self.me]

    def finish(self):
        def body(k, carry):
            source = lax.rem(self.me + self.devices - k, self.devices)
            self.copy(k, self.me, self.other(k)).wait_send()
            self.copy(k, source, self.me).wait_recv()
            return carry

        lax.fori_loop(1, self.devices, body, 0)


def turned(value, amount):
    return value if amount % LANES == 0 else pltpu.roll(value, amount % LANES, 1)


def lane_between(first, last):
    lane = lax.broadcasted_iota(jnp.int32, (8, LANES), 1)
    return (lane >= first) & (lane < last)


def put_tiles(out_ref, block, first, second, capacity):
    for k in range(LANES // capacity):
        tile = jnp.where(lane_between(0, capacity), turned(first, -k * capacity), 0.0)
        if second is not None:
            tile = jnp.where(
                lane_between(capacity, 2 * capacity), turned(second, capacity - k * capacity), tile
            )
        out_ref[block * (LANES // capacity) + k] = tile


def block_of(in_ref, block, capacity, half):
    total = jnp.zeros((8, LANES), jnp.float32)
    for k in range(LANES // capacity):
        tile = in_ref[block * (LANES // capacity) + k]
        total = jnp.where(
            lane_between(k * capacity, (k + 1) * capacity),
            turned(tile, (k - half) * capacity),
            total,
        )
    return total


def route_kernel(
    capacity, owner_hbm, cells_hbm, offsets_hbm, forces_hbm, slot_ref, table_ref, out_ref, in_ref,
    owner_ref, cells_ref, offsets_ref, forces_ref, load_sem, send_sem, recv_sem
):
    f32 = jnp.float32
    loads = [
        pltpu.make_async_copy(source, target, load_sem.at[k])
        for k, (source, target) in enumerate(
            (
                (owner_hbm, owner_ref), (cells_hbm, cells_ref), (offsets_hbm, offsets_ref),
                (forces_hbm, forces_ref),
            )
        )
    ]
    for copy in loads:
        copy.start()
    exchange = Exchange(out_ref, in_ref, send_sem, recv_sem)
    exchange.greet()
    for copy in loads:
        copy.wait()
    markers = owner_ref.shape[1]
    slots = capacity * exchange.devices
    owner = owner_ref[...].astype(f32)
    lanes = lax.broadcasted_iota(jnp.int32, (LANES, markers), 1)
    rows = lax.broadcasted_iota(jnp.int32, (LANES, markers), 0)
    before = jnp.zeros((8, markers), f32)
    for j in range(0, markers, LANES):
        group = jnp.broadcast_to(owner[:, j : j + LANES], (LANES, LANES))
        column = jnp.transpose(group)
        column = jnp.concatenate([column] * (markers // LANES), axis=1)
        same = jnp.where((column == owner) & (rows + j < lanes), 1.0, 0.0)
        for k in range(0, LANES, 8):
            before = before + same[k : k + 8]
    slot = (owner * capacity + jnp.sum(before, axis=0, keepdims=True)).astype(jnp.int32)
    slot_ref[...] = slot
    payload = jnp.concatenate(
        [
            cells_ref[...].astype(f32), offsets_ref[...], forces_ref[...],
            jnp.ones((1, markers), f32), jnp.zeros((6, markers), f32),
        ],
        axis=0,
    )
    split = thirds(payload)
    wide = 2 * LANES

    def pack(i, carry):
        place = lax.broadcasted_iota(jnp.int32, (wide, markers), 0) + i * wide
        sent = rejoined(transposed_dot(split, flags(place == slot)), 16)
        for k in range(2):
            part = sent[:, k * LANES : (k + 1) * LANES]
            put_tiles(out_ref, 2 * i + k, part[0:8], part[8:16], capacity)
        return carry

    lax.fori_loop(0, slots // wide, pack, 0)
    exchange.start()
    exchange.finish()

    def unpack(i, carry):
        table_ref[0:8, lanes_of(i)] = block_of(in_ref, i, capacity, 0)
        table_ref[8:16, lanes_of(i)] = block_of(in_ref, i, capacity, 1)
        return carry

    lax.fori_loop(0, slots // LANES, unpack, 0)


def routed(owner, cells, offsets, forces, capacity):
    devices = lax.axis_size("gx") * lax.axis_size("gy")
    markers = owner.shape[1]
    f32 = jnp.float32
    vmem = pl.BlockSpec(memory_space=pltpu.VMEM)
    return pl.pallas_call(
        functools.partial(route_kernel, capacity),
        out_shape=(
            jax.ShapeDtypeStruct((1, markers), jnp.int32),
            jax.ShapeDtypeStruct((16, devices * capacity), f32),
        ),
        in_specs=[pl.BlockSpec(memory_space=pltpu.HBM)] * 4,
        out_specs=[vmem] * 2,
        scratch_shapes=[pltpu.VMEM((devices, 8, LANES), f32)] * 2
        + [pltpu.VMEM((1, markers), jnp.int32), pltpu.VMEM((3, markers), jnp.int32)]
        + [pltpu.VMEM((3, markers), f32)] * 2
        + [pltpu.SemaphoreType.DMA((4,))]
        + [pltpu.SemaphoreType.DMA((devices,))] * 2,
        compiler_params=pltpu.CompilerParams(
            collective_id=1, has_side_effects=True, vmem_limit_bytes=24 * 1024 * 1024
        ),
    )(owner, cells, offsets, forces)


def sort_kernel(depth, size_x, received_ref, place_ref, table_ref):
    f32 = jnp.float32
    slots = received_ref.shape[1]
    tiles = depth // LANES
    blocks = slots // LANES
    valid = received_ref[9:10] > 0.5
    start = received_ref[2:3].astype(jnp.int32) - 1
    bins = jnp.where(start < 0, start + depth, start)
    bins = jnp.where(valid, lax.shift_right_logical(bins, LANES.bit_length() - 1), tiles)
    cell = received_ref[0:1].astype(jnp.int32)
    edge = valid & ((cell < SPREAD_ABOVE) | (cell >= size_x - SPREAD_BELOW))
    kinds = lax.broadcasted_iota(jnp.int32, (2 * tiles, slots), 0)
    member = jnp.where(kinds == 2 * bins + jnp.where(edge, 0, 1), 1.0, 0.0)
    stacked = jnp.concatenate(
        [member[:, b * LANES : (b + 1) * LANES] for b in range(blocks)], axis=0
    ).astype(jnp.bfloat16)
    above = lax.broadcasted_iota(jnp.int32, (LANES, LANES), 0) < lax.broadcasted_iota(
        jnp.int32, (LANES, LANES), 1
    )
    within = jnp.dot(stacked, flags(above), preferred_element_type=f32)
    sums = jnp.dot(stacked, jnp.ones((LANES, LANES), jnp.bfloat16), preferred_element_type=f32)
    ranks, run = [], jnp.zeros((2 * tiles, LANES), f32)
    for b in range(blocks):
        ranks.append(within[2 * b * tiles : 2 * (b + 1) * tiles] + run)
        run = run + sums[2 * b * tiles : 2 * (b + 1) * tiles]
    run = run.astype(jnp.int32)
    firsts, total = [], jnp.zeros((1, LANES), jnp.int32)
    lane = lax.broadcasted_iota(jnp.int32, (1, LANES), 1)
    tile_of, order, edge_total = jnp.zeros_like(total), jnp.zeros_like(total), total

    def chunks_for(amount):
        return lax.shift_right_logical(amount + (LANES - 1), LANES.bit_length() - 1)

    for k in range(tiles):
        edges, others = run[2 * k : 2 * k + 1], run[2 * k + 1 : 2 * k + 2]
        firsts += [total * LANES, total * LANES + edges]
        edge_chunks = chunks_for(edges)
        inside = (lane >= edge_total) & (lane < edge_total + edge_chunks)
        order = jnp.where(inside, total + lane - edge_total, order)
        edge_total = edge_total + edge_chunks
        total = total + chunks_for(edges + others)
        tile_of = tile_of + jnp.where(lane >= total, 1, 0)
    tile_of = jnp.minimum(tile_of, tiles - 1)
    order = jnp.where(lane >= edge_total, table_ref.shape[1] // LANES - 1, order)
    first = jnp.concatenate(firsts, axis=0).astype(f32)
    spots = jnp.concatenate(
        [
            jnp.sum(
                member[:, b * LANES : (b + 1) * LANES] * (ranks[b] + first), axis=0, keepdims=True
            )
            for b in range(blocks)
        ],
        axis=1,
    )
    place = jnp.where(valid, spots.astype(jnp.int32), -1)
    place_ref[...] = place
    count = jnp.max(total.astype(f32)).astype(jnp.int32)
    payload = jnp.concatenate(
        [
            received_ref[0:9], jnp.zeros((7, slots), f32),
        ],
        axis=0,
    )
    split = thirds(payload)
    table_ref[...] = jnp.zeros(table_ref.shape, f32)
    wide = 2 * LANES

    def gather(i, carry):
        spot = lax.broadcasted_iota(jnp.int32, (wide, slots), 0) + i * wide
        sorted_part = rejoined(transposed_dot(split, flags(spot == place)), 16)
        table_ref[:, pl.ds(pl.multiple_of(i * wide, wide), wide)] = sorted_part
        return carry

    lax.fori_loop(0, lax.div(count + 1, 2), gather, 0)
    for row, value in enumerate((tile_of, order, edge_total, total)):
        table_ref[12 + row : 13 + row, 0:LANES] = value.astype(f32)


def sorted_table(received, places, depth, size_x):
    vmem = pl.BlockSpec(memory_space=pltpu.VMEM)
    return pl.pallas_call(
        functools.partial(sort_kernel, depth, size_x),
        out_shape=(
            jax.ShapeDtypeStruct((1, received.shape[1]), jnp.int32),
            jax.ShapeDtypeStruct((16, places), jnp.float32),
        ),
        in_specs=[vmem],
        out_specs=[vmem] * 2,
        compiler_params=pltpu.CompilerParams(vmem_limit_bytes=16 * 1024 * 1024),
        cost_estimate=pl.CostEstimate(
            flops=3_000_000_000, bytes_accessed=1_000_000, transcendentals=0
        ),
    )(received)


def return_kernel(
    capacity, slot_ref, place_ref, own_ref, low_ref, high_ref, out_values_ref, out_ref, in_ref,
    marks_ref, back_ref, send_sem, recv_sem
):
    f32 = jnp.float32
    exchange = Exchange(out_ref, in_ref, send_sem, recv_sem)
    exchange.greet()
    slots, markers = marks_ref.shape
    places = own_ref.shape[1]
    wide = 2 * LANES
    place = place_ref[...]
    blank = jnp.zeros((5, wide), f32)

    def unsort(i, total):
        part = pl.ds(pl.multiple_of(i * wide, wide), wide)
        values = own_ref[:, part] + low_ref[:, part] + high_ref[:, part]
        split = thirds(jnp.concatenate([values, blank], axis=0))
        spot = lax.broadcasted_iota(jnp.int32, (wide, slots), 0) + i * wide
        return total + jnp.dot(split, flags(spot == place), preferred_element_type=f32)

    total = lax.fori_loop(0, places // wide, unsort, jnp.zeros((24, slots), f32))
    back_ref[...] = rejoined(total, 8)

    def pack(i, carry):
        put_tiles(out_ref, i, back_ref[:, lanes_of(i)], None, capacity)
        return carry

    lax.fori_loop(0, slots // LANES, pack, 0)
    exchange.start()
    slot = slot_ref[...]

    def mark(i, carry):
        rows = pl.ds(pl.multiple_of(i * LANES, LANES), LANES)
        here = lax.broadcasted_iota(jnp.int32, (LANES, markers), 0) + i * LANES
        marks_ref[rows, :] = flags(here == slot)
        return carry

    lax.fori_loop(0, slots // LANES, mark, 0)
    exchange.finish()

    def unpack(i, carry):
        back_ref[:, lanes_of(i)] = block_of(in_ref, i, capacity, 0)
        return carry

    lax.fori_loop(0, slots // LANES, unpack, 0)
    parts = jnp.dot(thirds(back_ref[...]), marks_ref[...], preferred_element_type=f32)
    out_values_ref[...] = rejoined(parts, 8)[0:3]


def given_back(slot, place, values, low_values, high_values, capacity):
    devices = lax.axis_size("gx") * lax.axis_size("gy")
    markers, slots = slot.shape[1], place.shape[1]
    f32 = jnp.float32
    vmem = pl.BlockSpec(memory_space=pltpu.VMEM)
    return pl.pallas_call(
        functools.partial(return_kernel, capacity),
        out_shape=jax.ShapeDtypeStruct((3, markers), f32),
        in_specs=[vmem] * 5,
        out_specs=vmem,
        scratch_shapes=[pltpu.VMEM((devices, 8, LANES), f32)] * 2
        + [pltpu.VMEM((slots, markers), jnp.bfloat16), pltpu.VMEM((8, slots), f32)]
        + [pltpu.SemaphoreType.DMA((devices,))] * 2,
        compiler_params=pltpu.CompilerParams(
            collective_id=2, has_side_effects=True, vmem_limit_bytes=24 * 1024 * 1024
        ),
    )(slot, place, values, low_values, high_values)


def tent(first, weights, length, wrap=0):
    rows = lax.broadcasted_iota(jnp.int32, (length, LANES), 0)
    table = jnp.zeros((length, LANES), jnp.float32)
    for j in range(4):
        target = first + j
        if wrap:
            target = jnp.where(target < 0, target + wrap, target)
            target = jnp.where(target >= wrap, target - wrap, target)
        table = table + jnp.where(rows == target, weights[j], 0.0)
    return table


def halves(value):
    high = value.astype(jnp.bfloat16)
    low = (value - high.astype(jnp.float32)).astype(jnp.bfloat16)
    return high, low


def chunk_tables(part, tile, x_shift, layers, ext_y, depth, marker_rows):
    cells = part[0:3].astype(jnp.int32)
    table_x = tent(cells[0:1] + x_shift, kernel_weights(part[3:4]), layers)
    table_y = tent(cells[1:2] - 1, kernel_weights(part[4:5]), ext_y, ext_y)
    start = cells[2:3] - 1
    start = jnp.where(start < 0, start + depth, start) - tile * LANES
    weights = kernel_weights(part[5:6])
    if not marker_rows:
        return table_x, table_y, tent(start, weights, 2 * LANES)
    packed = jnp.concatenate(
        [start.astype(jnp.float32), *weights, jnp.zeros((3, LANES), jnp.float32)], axis=0
    )
    columns = jnp.transpose(packed)
    where = lax.broadcasted_iota(jnp.int32, (LANES, 2 * LANES), 1).astype(jnp.float32)
    where = where - columns[:, 0:1]
    table_z = jnp.zeros((LANES, 2 * LANES), jnp.float32)
    for k in range(4):
        table_z = jnp.where(where == float(k), columns[:, k + 1 : k + 2], table_z)
    return table_x, table_y, table_z


def chunk_notes(tables, note_ref, note_sem):
    copies = [
        pltpu.make_async_copy(ref.at[8:16, 0:LANES], note_ref.at[k], note_sem.at[k])
        for k, ref in enumerate(tables)
    ]
    for copy in copies:
        copy.start()
    return copies


def note(note_ref, which, row, at):
    return note_ref[which, row, at].astype(jnp.int32)


def note_scratch(tables):
    return [pltpu.SMEM((tables, 8, LANES), jnp.float32), pltpu.SemaphoreType.DMA((tables,))]


def lanes_of(tile):
    return pl.ds(pl.multiple_of(tile * LANES, LANES), LANES)


def transposed_dot(left, right):
    return lax.dot_general(
        left, right, (((1,), (1,)), ((), ())), preferred_element_type=jnp.float32
    )


def padded(count):
    return -(-count // 8) * 8


def spread_kernel(shifts, together, *refs):
    tables, outs = refs[: len(shifts)], refs[len(shifts) : -2]
    note_ref, note_sem = refs[-2:]
    beside = len(tables) > 1
    copies = chunk_notes(tables, note_ref, note_sem)

    def clear(out_ref):
        def body(i, carry):
            for c in range(3):
                out_ref[c, i] = jnp.zeros(out_ref.shape[2:], jnp.float32)
            return carry

        lax.fori_loop(0, out_ref.shape[1], body, 0)

    for out_ref in outs:
        clear(out_ref)
    for copy in copies:
        copy.wait()

    groups = [(0, 1, 2)] if beside else [(0,), (1,), (2,)]

    def prepared(which, j):
        layers, ext_y, depth = outs[which].shape[1:]
        part = tables[which][:, lanes_of(j)]
        tile = note(note_ref, which, 4, j)
        table_x, table_y, table_z = chunk_tables(
            part, tile, shifts[which], padded(layers), ext_y, depth, True
        )
        z_high, z_low = halves(table_z)
        z_pair = jnp.concatenate([z_high, z_high], axis=0)
        after = lax.rem(tile + 1, depth // LANES)
        return outs[which], part, table_x, table_y, z_pair, z_low, tile, after

    def product(group, out_ref, part, table_x, table_y, z_pair, z_low, tile, after):
        planes = []
        for c in group:
            pushed = table_x * part[6 + c : 7 + c]
            planes += [pushed[x : x + 1] * table_y for x in range(out_ref.shape[1])]
        high, low = halves(jnp.concatenate(planes, axis=0))
        total = jnp.dot(
            jnp.concatenate([high, low], axis=1), z_pair, preferred_element_type=jnp.float32
        )
        return total + jnp.dot(high, z_low, preferred_element_type=jnp.float32)

    def add(group, step, total):
        out_ref, tile, after = step[0], step[-2], step[-1]
        layers, ext_y = out_ref.shape[1:3]
        shape = (len(group), layers, ext_y, LANES)
        these = slice(group[0], group[-1] + 1)
        out_ref[these, :, :, lanes_of(tile)] += total[:, :LANES].reshape(shape)
        out_ref[these, :, :, lanes_of(after)] += total[:, LANES:].reshape(shape)

    def chunk(j, carry):
        steps = [
            prepared(which, note(note_ref, which, 5, together * j + k) if beside else together * j + k)
            for which in range(len(tables))
            for k in range(together)
        ]
        for group in groups:
            for step in steps:
                add(group, step, product(group, *step))
        return carry

    counts = [note(note_ref, which, 6 if beside else 7, 0) for which in range(len(tables))]
    count = functools.reduce(jnp.maximum, counts)
    lax.fori_loop(0, lax.div(count + (together - 1), together), chunk, 0)


def spread_out(tables, shifts, layers, together, ext_y, depth, cost):
    return pl.pallas_call(
        functools.partial(spread_kernel, shifts, together),
        out_shape=[
            jax.ShapeDtypeStruct((3, count, ext_y, depth), jnp.float32) for count in layers
        ],
        in_specs=[pl.BlockSpec(memory_space=pltpu.VMEM)] * len(tables),
        out_specs=[pl.BlockSpec(memory_space=pltpu.VMEM)] * len(tables),
        scratch_shapes=note_scratch(len(tables)),
        compiler_params=pltpu.CompilerParams(vmem_limit_bytes=24 * 1024 * 1024),
        cost_estimate=pl.CostEstimate(flops=cost, bytes_accessed=1_000_000, transcendentals=0),
    )(*tables)


def smoothing_kernel(
    own_ref, below_ref, above_ref, vel_hbm, visc_hbm, vel_low, vel_high, out_ref, vel_ref,
    visc_ref, rhs_ref, field_a, field_b, fold_send, fold_recv, mid_send, mid_recv, rest_send,
    rest_recv, y_send, y_recv,
    last_send, last_recv, load_sem, send_sem, recv_sem
):
    size_x, size_y, depth = visc_hbm.shape
    ext_y = out_ref.shape[2]
    layers = size_x + 2
    tiles = depth // LANES
    count_x, count_y = lax.axis_size("gx"), lax.axis_size("gy")
    me_x, me_y = lax.axis_index("gx"), lax.axis_index("gy")
    x_up = (lax.rem(me_x + 1, count_x), me_y)
    x_down = (lax.rem(me_x + count_x - 1, count_x), me_y)
    y_up = (me_x, lax.rem(me_y + 1, count_y))
    y_down = (me_x, lax.rem(me_y + count_y - 1, count_y))

    loads = [
        pltpu.make_async_copy(source, target, load_sem.at[k])
        for k, (source, target) in enumerate(
            (
                (vel_low, vel_ref.at[:, 0:1]),
                (vel_high, vel_ref.at[:, size_x + 1 :]),
                (vel_hbm, vel_ref.at[:, 1 : size_x + 1]),
                (visc_hbm, visc_ref),
            )
        )
    ]
    for copy in loads:
        copy.start()

    barrier = pltpu.get_barrier_semaphore()
    for device in (x_up, x_down, y_up, y_down):
        pl.semaphore_signal(barrier, inc=1, device_id=device, device_id_type=MESH)
    pl.semaphore_wait(barrier, 4)

    used = [0]

    def send(source, target, device):
        sem = used[0]
        used[0] = sem + 1
        copy = pltpu.make_async_remote_copy(
            src_ref=source, dst_ref=target, send_sem=send_sem.at[sem], recv_sem=recv_sem.at[sem],
            device_id=device, device_id_type=MESH,
        )
        copy.start()
        return copy

    def wait(copies):
        for copy in copies:
            copy.wait()

    def row_of(ref, *index):
        return jnp.concatenate([ref[(*index, slice(t, t + 1))] for t in range(tiles)], axis=1)

    def set_row(ref, value, *index):
        for t in range(tiles):
            ref[(*index, slice(t, t + 1))] = value[:, t * LANES : (t + 1) * LANES]

    def build(x, beside=None, at=0):
        for c in range(3):
            plane = own_ref[c, x]
            if beside is not None:
                plane = plane + beside[c, x - at]
            inner = plane[0:size_y] + vel_ref[c, x]
            rhs_ref[c, x, size_y:ext_y, :] = plane[size_y:ext_y]
            rhs_ref[c, x, 0:size_y, :] = inner
            set_row(fold_send, inner[size_y - 1 : size_y], x, 0, c)
            set_row(fold_send, plane[size_y : size_y + 1], x, 1, c)
            set_row(fold_send, plane[size_y + 1 : size_y + 2], x, 2, c)
            set_row(fold_send, plane[ext_y - 1 : ext_y], x, 3, c)
            set_row(fold_send, inner[0:1], x, 4, c)

    def send_fold(first, count):
        part = pl.ds(first, count)
        return (
            send(fold_send.at[part, 0:3], fold_recv.at[part, 0:3], y_up),
            send(fold_send.at[part, 3:5], fold_recv.at[part, 3:5], y_down),
        )

    def fold(x, carry):
        for c in range(3):
            rhs_ref[c, x, 0:1, :] += row_of(fold_recv, x, 1, c)
            rhs_ref[c, x, 1:2, :] += row_of(fold_recv, x, 2, c)
            rhs_ref[c, x, size_y - 1 : size_y, :] += row_of(fold_recv, x, 3, c)
            rhs_ref[c, x, ext_y - 1 : ext_y, :] += row_of(fold_recv, x, 0, c)
            rhs_ref[c, x, size_y : size_y + 1, :] += row_of(fold_recv, x, 4, c)
        return carry

    below, above = below_ref.shape[1], above_ref.shape[1]

    def lower(x, carry):
        build(x, below_ref, 0)
        return carry

    def middle(x, carry):
        build(x)
        return carry

    def upper(x, carry):
        build(x, above_ref, layers - above)
        return carry

    wait(loads)
    lax.fori_loop(0, below, lower, 0)
    low_fold = send_fold(0, 3)
    lax.fori_loop(layers - above, layers, upper, 0)
    middle(layers - 3, 0)
    high_fold = send_fold(layers - 3, 3)
    lax.fori_loop(3, layers - 3, middle, 0)
    middle_fold = send_fold(3, layers - 6)

    top = 8 + mid_send.shape[2]

    def beside_plane(slot, c):
        rest = rest_recv[slot, c]
        return jnp.concatenate([rest[0:8], mid_recv[slot, c], rest[8:]], axis=0)

    def update(sweep, x, low=None, high=None, edge=None, early=False):
        visc = visc_ref[x]
        scale = 1.0 / (1.0 + 6.0 * visc)
        shift = 1 if sweep == 0 else 0
        current = (rhs_ref, field_a, field_b)[sweep]
        for c in range(3):
            wide = current[c, x + shift]
            total = pltpu.roll(wide, 1, 0) + pltpu.roll(wide, ext_y - 1, 0)
            total = total + pltpu.roll(wide, 1, 1) + pltpu.roll(wide, depth - 1, 1)
            before = current[c, x + shift - 1, 0:size_y, :] if low is None else beside_plane(low, c)
            behind = current[c, x + shift + 1, 0:size_y, :] if high is None else beside_plane(high, c)
            total = total[0:size_y] + before + behind
            plane = (rhs_ref[c, x + 1, 0:size_y, :] + visc * total) * scale
            if early:
                mid_send[2 * sweep + edge, c] = plane[8:top]
                continue
            if sweep == SWEEPS - 1:
                out_ref[c, x, 0:size_y, :] = plane
                set_row(last_send, plane[size_y - 1 : size_y], 0, x, c)
                set_row(last_send, plane[0:1], 1, x, c)
                set_row(last_send, plane[1:2], 2, x, c)
            else:
                (field_a, field_b)[sweep][c, x, 0:size_y, :] = plane
                set_row(y_send, plane[size_y - 1 : size_y], sweep, 0, x, c)
                set_row(y_send, plane[0:1], sweep, 1, x, c)
                if edge is not None:
                    rest_send[2 * sweep + edge, c, 0:8, :] = plane[0:8]
                    rest_send[2 * sweep + edge, c, 8:, :] = plane[top:]
                    if sweep:
                        mid_send[2 * sweep + edge, c] = plane[8:top]

    def interior(sweep):
        def body(x, carry):
            update(sweep, x)
            return carry

        lax.fori_loop(1, size_x - 1, body, 0)

    def send_x(sweep, way, mid):
        slot = 2 * sweep + way
        source, target = (mid_send, mid_recv) if mid else (rest_send, rest_recv)
        return send(source.at[slot], target.at[slot], (x_up, x_down)[way])

    def send_y(sweep, first, count):
        part = pl.ds(first, count)
        return (
            send(y_send.at[sweep, 0, part], y_recv.at[sweep, 0, part], y_up),
            send(y_send.at[sweep, 1, part], y_recv.at[sweep, 1, part], y_down),
        )

    def send_last(first, count):
        part = pl.ds(first, count)
        return (
            send(last_send.at[0, part], last_recv.at[0, part], y_up),
            send(last_send.at[1:3, part], last_recv.at[1:3, part], y_down),
        )

    def halo(sweep):
        field = (field_a, field_b)[sweep]

        def body(x, carry):
            for c in range(3):
                field[c, x, size_y : size_y + 1, :] = row_of(y_recv, sweep, 1, x, c)
                field[c, x, ext_y - 1 : ext_y, :] = row_of(y_recv, sweep, 0, x, c)
            return carry

        lax.fori_loop(0, size_x, body, 0)

    def halo_last(x, carry):
        for c in range(3):
            out_ref[c, x, size_y : size_y + 1, :] = row_of(last_recv, 1, x, c)
            out_ref[c, x, size_y + 1 : size_y + 2, :] = row_of(last_recv, 2, x, c)
            out_ref[c, x, size_y + 2 : ext_y - 1, :] = jnp.zeros(
                (ext_y - 3 - size_y, depth), jnp.float32
            )
            out_ref[c, x, ext_y - 1 : ext_y, :] = row_of(last_recv, 0, x, c)
        return carry

    update(0, 0, edge=1, early=True)
    x_copies = (send_x(0, 1, True),)
    update(0, size_x - 1, edge=0, early=True)
    x_copies = x_copies + (send_x(0, 0, True),)
    wait(low_fold)
    lax.fori_loop(0, 3, fold, 0)
    update(0, 0, edge=1)
    x_copies = x_copies + (send_x(0, 1, False),)
    wait(high_fold)
    lax.fori_loop(layers - 3, layers, fold, 0)
    update(0, size_x - 1, edge=0)
    x_copies = x_copies + (send_x(0, 0, False),)
    wait(middle_fold)
    lax.fori_loop(3, layers - 3, fold, 0)
    interior(0)
    y_copies = send_y(0, 0, size_x)
    wait(y_copies)
    halo(0)
    interior(1)
    y_copies = send_y(1, 1, size_x - 2)
    wait(x_copies)
    update(1, 0, low=0, edge=1)
    x_copies = (send_x(1, 1, True), send_x(1, 1, False))
    update(1, size_x - 1, high=1, edge=0)
    x_copies = x_copies + (send_x(1, 0, True), send_x(1, 0, False))
    y_copies = y_copies + send_y(1, 0, 1) + send_y(1, size_x - 1, 1)
    wait(y_copies)
    halo(1)
    interior(2)
    y_copies = send_last(1, size_x - 2)
    wait(y_copies)
    lax.fori_loop(1, size_x - 1, halo_last, 0)
    wait(x_copies)
    update(2, 0, low=2)
    y_copies = send_last(0, 1)
    update(2, size_x - 1, high=3)
    y_copies = y_copies + send_last(size_x - 1, 1)
    wait(y_copies)
    halo_last(0, 0)
    halo_last(size_x - 1, 0)


def smoothed(own, below, above, velocity, viscosity, vel_low, vel_high):
    size_x, size_y, depth = viscosity.shape
    ext_y = own.shape[2]
    layers = size_x + 2
    tiles = depth // LANES
    f32 = jnp.float32
    middle = size_y // 8 * 8 - 8
    vmem, hbm = pl.BlockSpec(memory_space=pltpu.VMEM), pl.BlockSpec(memory_space=pltpu.HBM)
    return pl.pallas_call(
        smoothing_kernel,
        out_shape=jax.ShapeDtypeStruct((3, size_x, ext_y, depth), f32),
        in_specs=[vmem] * 3 + [hbm] * 4,
        out_specs=vmem,
        scratch_shapes=[
            pltpu.VMEM((3, layers, size_y, depth), f32),
            pltpu.VMEM((size_x, size_y, depth), f32),
            pltpu.VMEM((3, layers, ext_y, depth), f32),
            pltpu.VMEM((3, size_x, ext_y, depth), f32),
            pltpu.VMEM((3, size_x, ext_y, depth), f32),
            pltpu.VMEM((layers, 5, 3, tiles, LANES), f32),
            pltpu.VMEM((layers, 5, 3, tiles, LANES), f32),
            pltpu.VMEM((4, 3, middle, depth), f32),
            pltpu.VMEM((4, 3, middle, depth), f32),
            pltpu.VMEM((4, 3, size_y - middle, depth), f32),
            pltpu.VMEM((4, 3, size_y - middle, depth), f32),
            pltpu.VMEM((2, 2, size_x, 3, tiles, LANES), f32),
            pltpu.VMEM((2, 2, size_x, 3, tiles, LANES), f32),
            pltpu.VMEM((3, size_x, 3, tiles, LANES), f32),
            pltpu.VMEM((3, size_x, 3, tiles, LANES), f32),
            pltpu.SemaphoreType.DMA((4,)),
            pltpu.SemaphoreType.DMA((28,)),
            pltpu.SemaphoreType.DMA((28,)),
        ],
        compiler_params=pltpu.CompilerParams(
            collective_id=0, has_side_effects=True, vmem_limit_bytes=32 * 1024 * 1024
        ),
    )(own, below, above, velocity, viscosity, vel_low, vel_high)


def sample_chunk(ref, tile, j, target, x_shift, high_of, low_of):
    layers, ext_y, depth = high_of.shape[1:]
    after = lax.rem(tile + 1, depth // LANES)
    table_x, table_y, table_z = chunk_tables(
        ref[:, lanes_of(j)], tile, x_shift, padded(layers), ext_y, depth, False
    )
    z_high, z_low = halves(table_z)
    z_pair = jnp.concatenate([z_high, z_low], axis=1)

    def window(ref):
        rows = (3 * layers * ext_y, LANES)
        return jnp.concatenate(
            [
                ref[:, :, :, lanes_of(tile)].reshape(rows),
                ref[:, :, :, lanes_of(after)].reshape(rows),
            ],
            axis=1,
        )

    pair = jnp.dot(window(high_of), z_pair, preferred_element_type=jnp.float32)
    columns = pair[:, :LANES] + pair[:, LANES:]
    columns = columns + jnp.dot(window(low_of), z_high, preferred_element_type=jnp.float32)
    for c in range(3):
        total = jnp.zeros((8, LANES), jnp.float32)
        for x in range(layers):
            at = (c * layers + x) * ext_y
            weighted = columns[at : at + ext_y] * table_y
            summed = weighted[0:8]
            for k in range(8, ext_y, 8):
                summed = summed + weighted[k : k + 8]
            total = total + summed * table_x[x : x + 1]
        target[c : c + 1, lanes_of(j)] = jnp.sum(total, axis=0, keepdims=True)


def sample_kernel(table_ref, field_ref, vel_ref, out_ref, field_high, field_low, note_ref, note_sem):
    size_x, size_y = vel_ref.shape[1:3]
    copies = chunk_notes([table_ref], note_ref, note_sem)

    def split(x, carry):
        for c in range(3):
            plane = field_ref[c, x]
            vel_ref[c, x] = plane[0:size_y]
            field_high[c, x], field_low[c, x] = halves(plane)
        return carry

    lax.fori_loop(0, size_x, split, 0)
    copies[0].wait()
    out_ref[...] = jnp.zeros(out_ref.shape, jnp.float32)

    def chunk(i, carry):
        for j in (2 * i, 2 * i + 1):
            tile = note(note_ref, 0, 4, j)
            sample_chunk(table_ref, tile, j, out_ref, -1, field_high, field_low)
        return carry

    lax.fori_loop(0, lax.div(note(note_ref, 0, 7, 0) + 1, 2), chunk, 0)


def sampled(table, field, size_y):
    size_x, ext_y, depth = field.shape[1:]
    f32 = jnp.float32
    vmem = pl.BlockSpec(memory_space=pltpu.VMEM)
    return pl.pallas_call(
        sample_kernel,
        out_shape=(
            jax.ShapeDtypeStruct((3, size_x, size_y, depth), f32),
            jax.ShapeDtypeStruct((3, table.shape[1]), f32),
        ),
        in_specs=[vmem] * 2,
        out_specs=[vmem] * 2,
        scratch_shapes=[pltpu.VMEM((3, size_x, ext_y, depth), jnp.bfloat16)] * 2
        + note_scratch(1),
        compiler_params=pltpu.CompilerParams(vmem_limit_bytes=28 * 1024 * 1024),
        cost_estimate=pl.CostEstimate(
            flops=10_000_000_000, bytes_accessed=1_000_000, transcendentals=0
        ),
    )(table, field)


def sample_beside_kernel(
    low_ref, high_ref, field_ref, low_out, high_out, first_high, first_low, last_high, last_low,
    note_ref, note_sem
):
    size_x = field_ref.shape[1]
    copies = chunk_notes([low_ref, high_ref], note_ref, note_sem)
    for c in range(3):
        for x in range(2):
            first_high[c, x], first_low[c, x] = halves(field_ref[c, x])
        last_high[c, 0], last_low[c, 0] = halves(field_ref[c, size_x - 1])
    for copy in copies:
        copy.wait()
    low_out[...] = jnp.zeros(low_out.shape, jnp.float32)
    high_out[...] = jnp.zeros(high_out.shape, jnp.float32)

    def chunk(i, carry):
        j = note(note_ref, 0, 5, i)
        tile = note(note_ref, 0, 4, j)
        sample_chunk(low_ref, tile, j, low_out, -size_x - 1, first_high, first_low)
        j = note(note_ref, 1, 5, i)
        tile = note(note_ref, 1, 4, j)
        sample_chunk(high_ref, tile, j, high_out, 0, last_high, last_low)
        return carry

    count = jnp.maximum(note(note_ref, 0, 6, 0), note(note_ref, 1, 6, 0))
    lax.fori_loop(0, count, chunk, 0)


def sampled_beside(low, high, field):
    ext_y, depth = field.shape[2:]
    vmem = pl.BlockSpec(memory_space=pltpu.VMEM)
    return pl.pallas_call(
        sample_beside_kernel,
        out_shape=[jax.ShapeDtypeStruct((3, low.shape[1]), jnp.float32)] * 2,
        in_specs=[vmem] * 3,
        out_specs=[vmem] * 2,
        scratch_shapes=[pltpu.VMEM((3, 2, ext_y, depth), jnp.bfloat16)] * 2
        + [pltpu.VMEM((3, 1, ext_y, depth), jnp.bfloat16)] * 2
        + note_scratch(2),
        compiler_params=pltpu.CompilerParams(vmem_limit_bytes=16 * 1024 * 1024),
        cost_estimate=pl.CostEstimate(
            flops=2_000_000_000, bytes_accessed=1_000_000, transcendentals=0
        ),
    )(low, high, field)


def stepped(velocity, viscosity, cells, offsets, forces, owners):
    rows_gx = lax.axis_size("gx")
    rows_gy = lax.axis_size("gy")
    devices = rows_gx * rows_gy
    markers = owners.shape[0]
    capacity = max(2, 2 * markers // devices)
    slots = capacity * devices
    size_x, size_y, depth = viscosity.shape
    ext_y = -(-(size_y + 3) // 8) * 8
    tiles = depth // LANES

    slot, received = routed(owners.reshape(1, markers), cells, offsets, forces, capacity)
    received, edge = lax.optimization_barrier((received, velocity[:, size_x - 1 :]))
    vel_low = shifted(edge, "gx", 1)
    chunks = -(-(slots // LANES + tiles) // 2) * 2
    place, own = sorted_table(received, chunks * LANES, depth, size_x)
    own, edge = lax.optimization_barrier((own, velocity[:, 0:1]))
    low = shifted(own, "gx", 1)
    high = shifted(own, "gx", -1)
    vel_high = shifted(edge, "gx", -1)
    (spread,) = spread_out([own], (0,), (size_x + 2,), 2, ext_y, depth, 10_000_000_000)
    below, above = spread_out(
        [low, high], (-size_x, 0), (SPREAD_BELOW, SPREAD_ABOVE), 2, ext_y, depth,
        2_000_000_000,
    )
    field = smoothed(spread, below, above, velocity, viscosity, vel_low, vel_high)
    low_values, high_values = sampled_beside(low, high, field)
    low_values = shifted(low_values, "gx", -1)
    high_values = shifted(high_values, "gx", 1)
    new_velocity, values = sampled(own, field, size_y)
    marker_velocity = given_back(slot, place, values, low_values, high_values, capacity)
    return (new_velocity, marker_velocity)


def solution(mesh):
    in_specs = (
        P(None, "gx", "gy", None),
        P("gx", "gy", None),
        P(None, ("gx", "gy")),
        P(None, ("gx", "gy")),
        P(None, ("gx", "gy")),
        P(("gx", "gy"), None),
    )
    out_specs = (P(None, "gx", "gy", None), P(None, ("gx", "gy")))
    return jax.shard_map(stepped, mesh=mesh, in_specs=in_specs, out_specs=out_specs, check_vma=False)
```
